32 devices in a mesh: groups: 2 (over y), ffn: 4 (over x, core), width: 4 (over z).
Axes of the slice: x: 2, y: 2, z: 4, core: 2. Of those that a mesh axis runs over, the one named last changes fastest.
Arguments:
- hidden: bfloat16 [2048, 8192], P(('groups', 'ffn'), 'width'), parts along dimension 0, may hold values from -8.4 to 8.4
- upstream: bfloat16 [2048, 8192], P(('groups', 'ffn'), 'width'), parts along dimension 0, may hold values from -6 to 6
- query_frozen_weight: bfloat16 [8192, 8192], P('width', 'ffn'), may hold values from -0.0625 to 0.0625
- key_value_frozen_weight: bfloat16 [2, 8192, 1024], P(None, 'width', 'ffn'), may hold values from -0.0625 to 0.0625
- output_frozen_weight: bfloat16 [8192, 8192], P('ffn', 'width'), may hold values from -0.0625 to 0.0625
- adapter_down: bfloat16 [6, 16, 8192], P('groups', None, 'width'), parts along dimension 0, may hold values from -0.0625 to 0.0625
- query_up_map: bfloat16 [32, 8192], P('groups', 'ffn'), parts along dimension 0, may hold values from -0.0625 to 0.0625
- key_value_up_maps: bfloat16 [4, 16, 1024], P('groups', None, 'ffn'), parts along dimension 0, may hold values from -0.0625 to 0.0625
- output_down_map: bfloat16 [32, 8192], P('groups', 'ffn'), parts along dimension 0, may hold values from -0.0625 to 0.0625
- output_up: bfloat16 [32, 8192], P('groups', 'width'), parts along dimension 0, may hold values from -0.0625 to 0.0625
Outputs:
- hidden_gradient: bfloat16 [2048, 8192], P(('groups', 'ffn'), 'width'), parts along dimension 0
- down_map_gradient: float32 [6, 16, 8192], P('groups', None, 'width'), parts along dimension 0
- query_up_map_gradient: float32 [32, 8192], P('groups', 'ffn'), parts along dimension 0
- key_value_up_maps_gradient: float32 [4, 16, 1024], P('groups', None, 'ffn'), parts along dimension 0
- output_down_map_gradient: float32 [32, 8192], P('groups', 'ffn'), parts along dimension 0
- output_up_map_gradient: float32 [32, 8192], P('groups', 'width'), parts along dimension 0
The draws below stay inside these ranges and needn't reach their ends.
There are 2 independent parts, one for each index of `groups`. The reference program is written for one: setup_inputs(seed, part) draws one part's arguments, and reference() takes and returns one part's arrays. A program takes and returns all parts, laid end to end along the dimension named above; an argument that names none is the same for every part. Nothing has to cross between parts.
All inputs are finite; a program needn't handle non-finite values.
Results may differ from the reference program's by a relative error of at most 0.04.
Values may be sent and summed in bfloat16 or wider, within the bound.
A program may use at most 128 MiB of HBM per device.

```python
import math
import jax
import jax.numpy as jnp
from jax import lax

MODEL_WIDTH = 8192
HEADS = 64
KV_HEADS = 8
HEAD_DIM = 128
ADAPTER_RANK = 16
TOKENS = 1024
N_FFN = 4
N_WIDTH = 4


def draw_hidden(key, part):
    base_key = jax.random.fold_in(jax.random.fold_in(key, 11), 0)
    values = jnp.clip(jax.random.normal(base_key, (TOKENS, MODEL_WIDTH), jnp.float32), -6.0, 6.0)
    return values.astype(jnp.bfloat16)


def steps_of(rng, dims, cuts, smallest, top_value):
    level = 1.0
    for dim, blocks in cuts:
        draws = jax.random.uniform(jax.random.fold_in(jax.random.fold_in(rng, 6), dim), (blocks,), jnp.float32, smallest / len(cuts), top_value / len(cuts))
        level = level * jnp.repeat(jnp.exp(draws), dims[dim] // blocks).reshape((-1,) + (1,) * (len(dims) - 1 - dim))
    return level


def normal_values(own_key, dims, scale, bound, cuts=(), held_as=jnp.bfloat16):
    drawn = scale * jax.random.normal(own_key, dims, jnp.float32)
    if cuts:
        drawn = drawn * steps_of(own_key, dims, cuts, -0.22, 0.18)
    return jnp.clip(drawn, -bound, bound).astype(held_as)


def setup_inputs(seed: int = 0, part: int = 0) -> dict:
    splits = jax.random.split(jax.random.key(seed), 11)
    own_keys = jax.random.split(jax.random.fold_in(splits[10], part), 11)
    return {
        "hidden": draw_hidden(jax.random.fold_in(jax.random.fold_in(splits[10], part), 71), part),
        "upstream": normal_values(own_keys[1], (TOKENS, MODEL_WIDTH), 1.0, 6.0, ((0, 4), (1, 4))),
        "query_frozen_weight": normal_values(splits[2], (MODEL_WIDTH, HEADS * HEAD_DIM), MODEL_WIDTH ** -0.5, 0.0625, ((0, 4), (1, 4))),
        "key_value_frozen_weight": normal_values(splits[3], (2, MODEL_WIDTH, KV_HEADS * HEAD_DIM), MODEL_WIDTH ** -0.5, 0.0625, ((1, 4), (2, 4))),
        "output_frozen_weight": normal_values(splits[4], (HEADS * HEAD_DIM, MODEL_WIDTH), (HEADS * HEAD_DIM) ** -0.5, 0.0625, ((0, 4), (1, 4))),
        "adapter_down": normal_values(own_keys[5], (3, ADAPTER_RANK, MODEL_WIDTH), MODEL_WIDTH ** -0.5, 0.0625, ((2, 4),)),
        "query_up_map": normal_values(own_keys[6], (ADAPTER_RANK, HEADS * HEAD_DIM), MODEL_WIDTH ** -0.5, 0.0625, ((1, 4),)),
        "key_value_up_maps": normal_values(own_keys[7], (2, ADAPTER_RANK, KV_HEADS * HEAD_DIM), MODEL_WIDTH ** -0.5, 0.0625, ((2, 4),)),
        "output_down_map": normal_values(own_keys[8], (ADAPTER_RANK, HEADS * HEAD_DIM), (HEADS * HEAD_DIM) ** -0.5, 0.0625, ((1, 4),)),
        "output_up": normal_values(own_keys[9], (ADAPTER_RANK, MODEL_WIDTH), MODEL_WIDTH ** -0.5, 0.0625, ((1, 4),)),
    }


adapter_scale = 2.0
rope_base = 500000.0

def rotate(values, positions, first_dim, direction):
    columns = values.shape[1]
    head_dims = (first_dim + jnp.arange(columns, dtype=jnp.int32)) % HEAD_DIM
    pair_dims = head_dims - head_dims % 2
    frequency = jnp.exp(pair_dims.astype(jnp.float32) * (-math.log(rope_base) / HEAD_DIM))
    angles = positions.astype(jnp.float32)[:, None] * frequency[None, :]
    is_even = head_dims % 2 == 0
    following = jnp.roll(values, -1, axis=1)
    preceding = jnp.roll(values, 1, axis=1)
    partner = jnp.where(is_even[None, :], -following, preceding)
    return values * jnp.cos(angles) + direction * partner * jnp.sin(angles)

def width_grouped(left_side, right_side):
    block_size = left_side.shape[1] // N_WIDTH
    running = jnp.zeros((left_side.shape[0], right_side.shape[1]), jnp.float32)
    for block_index in range(N_WIDTH):
        offset = block_index * block_size
        partial_value = jnp.dot(left_side[:, offset:offset + block_size], right_side[offset:offset + block_size, :], preferred_element_type=jnp.float32)
        running = running + lax.optimization_barrier(partial_value.astype(jnp.bfloat16)).astype(jnp.float32)
    return running

def head_grouped(contraction_pairs, token_count):
    running = jnp.zeros((token_count, MODEL_WIDTH), jnp.float32)
    for block_index in range(N_FFN):
        partial_value = jnp.zeros((token_count, MODEL_WIDTH), jnp.float32)
        for gradient, weight in contraction_pairs:
            block_size = weight.shape[1] // N_FFN
            offset = block_index * block_size
            partial_value = partial_value + jnp.dot(gradient[:, offset:offset + block_size], weight[:, offset:offset + block_size].T, preferred_element_type=jnp.float32)
        running = running + lax.optimization_barrier(partial_value.astype(jnp.bfloat16)).astype(jnp.float32)
    return running

def reference(hidden, upstream, query_frozen_weight, key_value_frozen_weight, output_frozen_weight, adapter_down, query_up_map, key_value_up_maps, output_down_map, output_up):
    token_count = hidden.shape[0]
    group_size = HEADS // KV_HEADS
    score_scale = 1.0 / math.sqrt(HEAD_DIM)
    positions = jnp.arange(token_count, dtype=jnp.int32)
    down_flattened = adapter_down.reshape(3 * ADAPTER_RANK, MODEL_WIDTH)
    reduced_hidden = jnp.dot(hidden, down_flattened.T, preferred_element_type=jnp.float32).astype(jnp.bfloat16)
    reduced_query = reduced_hidden[:, :ADAPTER_RANK]
    reduced_key = reduced_hidden[:, ADAPTER_RANK:2 * ADAPTER_RANK]
    reduced_value = reduced_hidden[:, 2 * ADAPTER_RANK:]
    output_reduced = jnp.dot(upstream, output_up.T, preferred_element_type=jnp.float32).astype(jnp.bfloat16)
    query_projected = width_grouped(hidden, query_frozen_weight) + adapter_scale * jnp.dot(reduced_query, query_up_map, preferred_element_type=jnp.float32)
    query_states = rotate(query_projected, positions, 0, 1.0).astype(jnp.bfloat16)
    key_projected = width_grouped(hidden, key_value_frozen_weight[0]) + adapter_scale * jnp.dot(reduced_key, key_value_up_maps[0], preferred_element_type=jnp.float32)
    key_states = rotate(key_projected, positions, 0, 1.0).astype(jnp.bfloat16)
    value_state_rows = (width_grouped(hidden, key_value_frozen_weight[1]) + adapter_scale * jnp.dot(reduced_value, key_value_up_maps[1], preferred_element_type=jnp.float32)).astype(jnp.bfloat16)
    attention_output_gradient = (width_grouped(upstream, output_frozen_weight.T) + adapter_scale * jnp.dot(output_reduced, output_down_map, preferred_element_type=jnp.float32)).astype(jnp.bfloat16)
    query_heads = query_states.reshape(token_count, KV_HEADS, group_size, HEAD_DIM).transpose(1, 0, 2, 3)
    grad_heads = attention_output_gradient.reshape(token_count, KV_HEADS, group_size, HEAD_DIM).transpose(1, 0, 2, 3)
    key_heads = key_states.reshape(token_count, KV_HEADS, HEAD_DIM).transpose(1, 0, 2)
    value_heads = value_state_rows.reshape(token_count, KV_HEADS, HEAD_DIM).transpose(1, 0, 2)
    causal = positions[:, None] >= positions[None, :]

    def one_head(head_items):
        query_one = head_items[0].astype(jnp.float32)
        key_one = head_items[1].astype(jnp.float32)
        value_one = head_items[2].astype(jnp.float32)
        grad_one = head_items[3].astype(jnp.float32)
        scores = jnp.einsum('tgd,sd->gts', query_one, key_one) * score_scale
        scores = jnp.where(causal[None, :, :], scores, -jnp.inf)
        shifted = jnp.exp(scores - lax.optimization_barrier(jnp.max(scores, axis=-1, keepdims=True)))
        probs = shifted / lax.optimization_barrier(jnp.sum(shifted, axis=-1, keepdims=True))
        prob_weights = lax.optimization_barrier(probs.astype(jnp.bfloat16)).astype(jnp.float32)
        attention_one = jnp.einsum('gts,sd->tgd', prob_weights, value_one).astype(jnp.bfloat16)
        prob_grad = jnp.einsum('tgd,sd->gts', grad_one, value_one)
        delta = jnp.einsum('tgd,tgd->gt', grad_one, attention_one.astype(jnp.float32))
        score_grad = lax.optimization_barrier((probs * (prob_grad - delta[:, :, None]) * score_scale).astype(jnp.bfloat16)).astype(jnp.float32)
        query_rot = jnp.einsum('gts,sd->tgd', score_grad, key_one)
        key_rot = jnp.einsum('gts,tgd->sd', score_grad, query_one)
        value_grad = jnp.einsum('gts,tgd->sd', prob_weights, grad_one)
        return (attention_one, query_rot, key_rot, value_grad)
    attention_heads, query_rots, key_rots, value_grads = lax.map(one_head, (query_heads, key_heads, value_heads, grad_heads))
    attention_output = attention_heads.transpose(1, 0, 2, 3).reshape(token_count, HEADS * HEAD_DIM)
    query_rot_all = query_rots.transpose(1, 0, 2, 3).reshape(token_count, HEADS * HEAD_DIM)
    key_rot_all = key_rots.transpose(1, 0, 2).reshape(token_count, KV_HEADS * HEAD_DIM)
    value_all = value_grads.transpose(1, 0, 2).reshape(token_count, KV_HEADS * HEAD_DIM)
    query_rows_gradient = rotate(query_rot_all, positions, 0, -1.0).astype(jnp.bfloat16)
    key_rows_gradient = rotate(key_rot_all, positions, 0, -1.0).astype(jnp.bfloat16)
    value_rows_gradient = value_all.astype(jnp.bfloat16)
    rank_gradient = jnp.concatenate([jnp.dot(query_rows_gradient, query_up_map.T, preferred_element_type=jnp.float32), jnp.dot(key_rows_gradient, key_value_up_maps[0].T, preferred_element_type=jnp.float32), jnp.dot(value_rows_gradient, key_value_up_maps[1].T, preferred_element_type=jnp.float32)], axis=1).astype(jnp.bfloat16)
    contraction_pairs = ((query_rows_gradient, query_frozen_weight), (key_rows_gradient, key_value_frozen_weight[0]), (value_rows_gradient, key_value_frozen_weight[1]))
    hidden_gradient_total = head_grouped(contraction_pairs, token_count) + adapter_scale * jnp.dot(rank_gradient, down_flattened, preferred_element_type=jnp.float32)
    hidden_gradient = hidden_gradient_total.astype(jnp.bfloat16)
    down_map_gradient = (adapter_scale * jnp.dot(rank_gradient.T, hidden, preferred_element_type=jnp.float32)).reshape(3, ADAPTER_RANK, MODEL_WIDTH)
    query_up_map_gradient = adapter_scale * jnp.dot(reduced_query.T, query_rows_gradient, preferred_element_type=jnp.float32)
    key_value_up_maps_gradient = adapter_scale * jnp.stack([jnp.dot(reduced_key.T, key_rows_gradient, preferred_element_type=jnp.float32), jnp.dot(reduced_value.T, value_rows_gradient, preferred_element_type=jnp.float32)])
    outer_product_rank = jnp.dot(attention_output, output_down_map.T, preferred_element_type=jnp.float32).astype(jnp.bfloat16)
    output_down_map_gradient = adapter_scale * jnp.dot(output_reduced.T, attention_output, preferred_element_type=jnp.float32)
    output_up_map_gradient = adapter_scale * jnp.dot(outer_product_rank.T, upstream, preferred_element_type=jnp.float32)
    return (hidden_gradient, down_map_gradient, query_up_map_gradient, key_value_up_maps_gradient, output_down_map_gradient, output_up_map_gradient)
```

```python
import functools
import math

import jax
import jax.numpy as jnp
import numpy as np
from jax import lax
from jax.experimental import pallas as pl
from jax.experimental.pallas import tpu as pltpu
from jax.sharding import PartitionSpec as P

KV_HEADS = 8
HEAD_DIM = 128
ADAPTER_RANK = 16
CHUNK_HEADS = 2
BLOCKS = 4
LAG = 3
BACK_LAG = 2
MESH = pl.DeviceIdType.MESH
LAST = (((1,), (1,)), ((), ()))
FIRST = (((0,), (0,)), ((), ()))


adapter_scale = 2.0
rope_base = 500000.0


def from_partner(array, axis, bit):
    return lax.ppermute(array, axis, [(i, i ^ 1 << bit) for i in range(lax.axis_size(axis))])


def rotate(values, positions, first_dim, direction):
    columns = values.shape[1]
    head_dims = (first_dim + jnp.arange(columns, dtype=jnp.int32)) % HEAD_DIM
    pair_dims = head_dims - head_dims % 2
    frequency = jnp.exp(pair_dims.astype(jnp.float32) * (-math.log(rope_base) / HEAD_DIM))
    angles = positions.astype(jnp.float32)[:, None] * frequency[None, :]
    is_even = head_dims % 2 == 0
    following = jnp.roll(values, -1, axis=1)
    preceding = jnp.roll(values, 1, axis=1)
    partner = jnp.where(is_even[None, :], -following, preceding)
    return values * jnp.cos(angles) + direction * partner * jnp.sin(angles)


def contract_last(left_side, right_side):
    return lax.dot_general(
        left_side, right_side, (((1,), (1,)), ((), ())), preferred_element_type=jnp.float32
    )


def contract_leading(left_side, right_side):
    return lax.dot_general(
        left_side, right_side, (((0,), (0,)), ((), ())), preferred_element_type=jnp.float32
    )


def shards(
    hidden,
    upstream,
    query_frozen_weight,
    key_value_frozen_weight,
    output_frozen_weight,
    adapter_down,
    query_up_map,
    key_value_up_maps,
    output_down_map,
    output_up,
):
    ffn_count = lax.axis_size("ffn")
    width_count = lax.axis_size("width")
    ffn_index = lax.axis_index("ffn")
    width_index = lax.axis_index("width")
    hidden_rows_full, upstream_gradient_full = (
        lax.all_gather(hidden, "ffn", axis=0, tiled=True),
        lax.all_gather(upstream, "ffn", axis=0, tiled=True),
    )
    token_count = hidden_rows_full.shape[0]
    query_rows = token_count // width_count
    query_cols = query_frozen_weight.shape[1]
    key_cols = key_value_frozen_weight.shape[2]
    row_start = width_index * query_rows
    positions = jnp.arange(token_count, dtype=jnp.int32)
    row_positions = row_start + jnp.arange(query_rows, dtype=jnp.int32)
    query_offset = ffn_index * query_cols
    key_offset = ffn_index * key_cols
    score_scale = 1.0 / math.sqrt(HEAD_DIM)
    down_flattened = adapter_down.reshape(3 * ADAPTER_RANK, adapter_down.shape[2])
    paired = ffn_count > KV_HEADS
    parity = ffn_index % 2
    rank_terms = contract_last(hidden_rows_full, down_flattened)
    upstream_terms = contract_last(upstream_gradient_full, output_up)
    rank_sum, upstream_sum = lax.psum((rank_terms, upstream_terms), "width")
    reduced_hidden = rank_sum.astype(jnp.bfloat16)
    output_reduced = upstream_sum.astype(jnp.bfloat16)
    low_rows = lax.dynamic_slice_in_dim(reduced_hidden, row_start, query_rows, 0)
    output_token_rows = lax.dynamic_slice_in_dim(output_reduced, row_start, query_rows, 0)
    query_part = jnp.dot(hidden_rows_full, query_frozen_weight, preferred_element_type=jnp.float32)
    query_gradient_summed = lax.psum_scatter(
        query_part.astype(jnp.bfloat16), "width", scatter_dimension=0, tiled=True
    ).astype(jnp.float32)
    query_projected = query_gradient_summed + adapter_scale * jnp.dot(
        low_rows[:, :ADAPTER_RANK], query_up_map, preferred_element_type=jnp.float32
    )
    query_states = rotate(query_projected, row_positions, query_offset, 1.0).astype(jnp.bfloat16)
    key_part = jnp.dot(
        hidden_rows_full, key_value_frozen_weight[0], preferred_element_type=jnp.float32
    )
    value_part = jnp.dot(
        hidden_rows_full, key_value_frozen_weight[1], preferred_element_type=jnp.float32
    )
    key_gradient_summed, value_gradient_summed = (
        lax.psum_scatter(
            key_part.astype(jnp.bfloat16), "width", scatter_dimension=0, tiled=True
        ).astype(jnp.float32),
        lax.psum_scatter(
            value_part.astype(jnp.bfloat16), "width", scatter_dimension=0, tiled=True
        ).astype(jnp.float32),
    )
    key_projected = key_gradient_summed + adapter_scale * jnp.dot(
        low_rows[:, ADAPTER_RANK : 2 * ADAPTER_RANK],
        key_value_up_maps[0],
        preferred_element_type=jnp.float32,
    )
    value_projected = value_gradient_summed + adapter_scale * jnp.dot(
        low_rows[:, 2 * ADAPTER_RANK :], key_value_up_maps[1], preferred_element_type=jnp.float32
    )
    key_block = rotate(key_projected, row_positions, key_offset, 1.0).astype(jnp.bfloat16)
    value_block = value_projected.astype(jnp.bfloat16)
    key_states, value_state_rows = (
        lax.all_gather(key_block, "width", axis=0, tiled=True),
        lax.all_gather(value_block, "width", axis=0, tiled=True),
    )
    if paired:
        other_key, other_value = from_partner((key_states, value_state_rows), "ffn", 0)
        key_states = jnp.where(
            parity == 0,
            jnp.concatenate([key_states, other_key], 1),
            jnp.concatenate([other_key, key_states], 1),
        )
        value_state_rows = jnp.where(
            parity == 0,
            jnp.concatenate([value_state_rows, other_value], 1),
            jnp.concatenate([other_value, value_state_rows], 1),
        )
    local_heads = query_cols // HEAD_DIM
    local_groups = key_states.shape[1] // HEAD_DIM
    group_size = local_heads // local_groups
    query_four = query_states.reshape(query_rows, local_groups, group_size, HEAD_DIM)
    key_three = key_states.reshape(token_count, local_groups, HEAD_DIM)
    value_three = value_state_rows.reshape(token_count, local_groups, HEAD_DIM)
    causal = row_positions[:, None] >= positions[None, :]
    scores = (
        jnp.einsum("qkgd,skd->kgqs", query_four, key_three, preferred_element_type=jnp.float32)
        * score_scale
    )
    scores = jnp.where(causal[None, None, :, :], scores, -jnp.inf)
    shifted = jnp.exp(scores - jnp.max(scores, axis=-1, keepdims=True))
    probs = shifted / jnp.sum(shifted, axis=-1, keepdims=True)
    prob_weights = probs.astype(jnp.bfloat16)
    attention_four = jnp.einsum(
        "kgqs,skd->qkgd", prob_weights, value_three, preferred_element_type=jnp.float32
    ).astype(jnp.bfloat16)
    attention_output = attention_four.reshape(query_rows, query_cols)
    out_part = contract_last(upstream_gradient_full, output_frozen_weight)
    output_gradient_summed = lax.psum_scatter(
        out_part.astype(jnp.bfloat16), "width", scatter_dimension=0, tiled=True
    ).astype(jnp.float32)
    attention_output_gradient = (
        output_gradient_summed
        + adapter_scale
        * jnp.dot(output_token_rows, output_down_map, preferred_element_type=jnp.float32)
    ).astype(jnp.bfloat16)
    grad_four = attention_output_gradient.reshape(query_rows, local_groups, group_size, HEAD_DIM)
    prob_grad = jnp.einsum(
        "qkgd,skd->kgqs", grad_four, value_three, preferred_element_type=jnp.float32
    )
    delta = jnp.einsum(
        "qkgd,qkgd->kgq", grad_four, attention_four, preferred_element_type=jnp.float32
    )
    score_grad = (probs * (prob_grad - delta[:, :, :, None]) * score_scale).astype(jnp.bfloat16)
    query_rot_grad = jnp.einsum(
        "kgqs,skd->qkgd", score_grad, key_three, preferred_element_type=jnp.float32
    ).reshape(query_rows, query_cols)
    key_part_grad = jnp.einsum(
        "kgqs,qkgd->skd", score_grad, query_four, preferred_element_type=jnp.float32
    ).reshape(token_count, local_groups * HEAD_DIM)
    value_part_grad = jnp.einsum(
        "kgqs,qkgd->skd", prob_weights, grad_four, preferred_element_type=jnp.float32
    ).reshape(token_count, local_groups * HEAD_DIM)
    query_block_grad = rotate(query_rot_grad, row_positions, query_offset, -1.0).astype(
        jnp.bfloat16
    )

    def own_half(values):
        return lax.dynamic_slice_in_dim(values, parity * key_cols, key_cols, 1)

    def other_half(values):
        return lax.dynamic_slice_in_dim(values, (1 - parity) * key_cols, key_cols, 1)

    key_total, value_total = lax.psum((key_part_grad, value_part_grad), "width")
    if paired:
        sent_key, sent_value = from_partner(
            (other_half(key_total), other_half(value_total)), "ffn", 0
        )
        key_total = own_half(key_total) + sent_key
        value_total = own_half(value_total) + sent_value
    key_rows_gradient = rotate(key_total, positions, key_offset, -1.0).astype(jnp.bfloat16)
    value_rows_gradient = value_total.astype(jnp.bfloat16)
    query_rows_gradient = lax.all_gather(query_block_grad, "width", axis=0, tiled=True)
    input_part = (
        contract_last(query_rows_gradient, query_frozen_weight)
        + contract_last(key_rows_gradient, key_value_frozen_weight[0])
        + contract_last(value_rows_gradient, key_value_frozen_weight[1])
    )
    rank_grad_terms = jnp.concatenate(
        [
            contract_last(query_rows_gradient, query_up_map),
            contract_last(key_rows_gradient, key_value_up_maps[0]),
            contract_last(value_rows_gradient, key_value_up_maps[1]),
        ],
        axis=1,
    )
    rank_gradient = lax.psum(rank_grad_terms, "ffn").astype(jnp.bfloat16)
    input_sum = lax.psum_scatter(
        input_part.astype(jnp.bfloat16), "ffn", scatter_dimension=0, tiled=True
    ).astype(jnp.float32)
    own_rows = token_count // ffn_count
    rank_gradient_token_rows = lax.dynamic_slice_in_dim(
        rank_gradient, ffn_index * own_rows, own_rows, 0
    )
    hidden_gradient = (
        input_sum
        + adapter_scale
        * jnp.dot(rank_gradient_token_rows, down_flattened, preferred_element_type=jnp.float32)
    ).astype(jnp.bfloat16)
    down_map_gradient = (adapter_scale * contract_leading(rank_gradient, hidden_rows_full)).reshape(
        adapter_down.shape
    )
    query_up_map_gradient = adapter_scale * contract_leading(
        reduced_hidden[:, :ADAPTER_RANK], query_rows_gradient
    )
    key_value_up_maps_gradient = adapter_scale * jnp.stack(
        [
            contract_leading(reduced_hidden[:, ADAPTER_RANK : 2 * ADAPTER_RANK], key_rows_gradient),
            contract_leading(reduced_hidden[:, 2 * ADAPTER_RANK :], value_rows_gradient),
        ]
    )
    outer_terms = contract_last(attention_output, output_down_map)
    outer_rows = lax.psum(outer_terms, "ffn").astype(jnp.bfloat16)
    outer_product_rank = lax.all_gather(outer_rows, "width", axis=0, tiled=True)
    output_down_map_gradient = adapter_scale * lax.psum(
        contract_leading(output_token_rows, attention_output), "width"
    )
    output_up_map_gradient = adapter_scale * contract_leading(
        outer_product_rank, upstream_gradient_full
    )
    return (
        hidden_gradient,
        down_map_gradient,
        query_up_map_gradient,
        key_value_up_maps_gradient,
        output_down_map_gradient,
        output_up_map_gradient,
    )


def dot(left, right, dims=None):
    if dims is None:
        return jnp.dot(left, right, preferred_element_type=jnp.float32)
    return lax.dot_general(left, right, dims, preferred_element_type=jnp.float32)


def other_index(a, b):
    low = lax.rem(lax.rem(a, 2) + lax.rem(b, 2), 2)
    high = lax.rem(lax.div(a, 2) + lax.div(b, 2), 2)
    return 2 * high + low


def fused(
    score_scale,
    hidden_in, upstream_in, query_weight, key_value_weight, output_weight,
    cosine, sine, down, query_up, key_value_up, output_down, output_up,
    hidden_out, down_out, query_up_out, key_value_up_out, output_down_out, output_up_out,
    hid, up, wh, wg, buf, own, back, acc, land, tmp, key_state, value_state, key_grad, value_grad,
    low_own, low_sent, low_got, low, rank_sum, rank_pair, rank_got, outer, outer_pair, outer_got, misc,
    query_acc, key_value_acc,
    load_sem, weight_sem, grad_sem, gather_send, gather_recv, send_sem, recv_sem, back_send, back_recv,
    low_send, low_recv, misc_send, misc_recv, outer_send, outer_recv, land_send, land_recv,
    rank_send, rank_recv,
):
    bf16, f32 = jnp.bfloat16, jnp.float32
    rows, width = hidden_in.shape
    cols = CHUNK_HEADS * HEAD_DIM
    chunks = wh.shape[1] - 1
    side_cols = chunks * cols
    rank = ADAPTER_RANK
    pieces = 4 + 8 * chunks
    back_pieces = 4 * chunks + 4
    tiles = width // cols
    f = lax.axis_index("ffn")
    z = lax.axis_index("width")
    half = lax.div(z, 2)
    ahead = 1 - 2 * half
    inner = z + ahead
    outward = z - ahead
    is_end = (z == 0) | (z == 3)
    is_mid = (z == 1) | (z == 2)
    core_peer = f + 1 - 2 * lax.rem(f, 2)
    chip_peer = lax.rem(f + 2, 4)

    def copy(src, dst, send, recv, axis, target):
        return pltpu.make_async_remote_copy(
            src_ref=src, dst_ref=dst, send_sem=send, recv_sem=recv,
            device_id={axis: target}, device_id_type=MESH,
        )

    def side_of(side):
        return half + side * (1 - 2 * half)

    def loop(count, step, start=0):
        def run(i, carry):
            step(i)
            return carry
        lax.fori_loop(start, count, run, 0)

    load_hidden = pltpu.make_async_copy(hidden_in, hid.at[0], load_sem.at[0])
    load_upstream = pltpu.make_async_copy(upstream_in, up.at[0], load_sem.at[1])

    def load_weight(side, c):
        start = pl.multiple_of(side_of(side) * side_cols + c * cols, cols)
        return pltpu.make_async_copy(
            query_weight.at[:, pl.ds(start, cols)], wh.at[side, c], weight_sem.at[side, c]
        )

    def load_key_value(side, which):
        start = pl.multiple_of(side_of(side) * HEAD_DIM, HEAD_DIM)
        return pltpu.make_async_copy(
            key_value_weight.at[which, :, pl.ds(start, HEAD_DIM)],
            wh.at[side, chunks, :, pl.ds(which * HEAD_DIM, HEAD_DIM)],
            weight_sem.at[side, chunks + which],
        )

    def load_grad_weight(side, fetch):
        start = pl.multiple_of(side_of(side) * side_cols + lax.rem(fetch, chunks) * cols, cols)
        slot = lax.rem(fetch, 2)
        return pltpu.make_async_copy(
            output_weight.at[pl.ds(start, cols), :], wg.at[slot, side], grad_sem.at[slot, side]
        )

    load_hidden.start()
    for side in range(2):
        for which in range(2):
            load_key_value(side, which).start()
    for c in range(chunks):
        for side in range(2):
            load_weight(side, c).start()
    load_upstream.start()
    for fetch in range(2):
        for side in range(2):
            load_grad_weight(side, fetch).start()

    barrier = pltpu.get_barrier_semaphore()
    pl.semaphore_signal(barrier, inc=1, device_id={"ffn": core_peer}, device_id_type=MESH)
    pl.semaphore_signal(barrier, inc=1, device_id={"ffn": chip_peer}, device_id_type=MESH)
    pl.semaphore_signal(barrier, inc=1, device_id={"width": inner}, device_id_type=MESH)

    @pl.when(is_mid)
    def _():
        pl.semaphore_signal(barrier, inc=1, device_id={"width": outward}, device_id_type=MESH)
        pl.semaphore_wait(barrier, 4)

    @pl.when(is_end)
    def _():
        pl.semaphore_wait(barrier, 3)

    def gather(which, kind):
        source, full = ((hidden_in, hid), (upstream_in, up))[which]
        sems = gather_send.at[which, kind], gather_recv.at[which, kind]
        if kind == 0:
            return copy(source, full.at[1], *sems, "ffn", core_peer)
        if kind == 1:
            return copy(source, full.at[2], *sems, "ffn", chip_peer)
        return copy(full.at[2], full.at[3], *sems, "ffn", core_peer)

    for which in range(2):
        gather(which, 1).start()
        gather(which, 0).start()

    def send_away_end(s):
        return copy(buf.at[1, s], buf.at[1, s], send_sem.at[1, s], recv_sem.at[1, s], "width", inner)

    def send_away_mid(s):
        return copy(buf.at[1, s], buf.at[0, s], send_sem.at[1, s], recv_sem.at[0, s], "width", inner)

    def send_home(s):
        return copy(buf.at[0, s], buf.at[0, s], send_sem.at[0, s], recv_sem.at[0, s], "width", outward)

    def arrived(side, s):
        copy(
            buf.at[side, s], buf.at[side, s], send_sem.at[side, s], recv_sem.at[side, s], "width", inner
        ).wait_recv()

    def relay_home(s):
        arrived(0, s)
        buf[0, s] = (buf[0, s].astype(f32) + own[s].astype(f32)).astype(bf16)
        send_home(s).start()

    def push(s):
        @pl.when(is_end)
        def _():
            buf[1, s] = tmp[...].astype(bf16)
            send_away_end(s).start()

        @pl.when(is_mid)
        def _():
            arrived(1, s)
            buf[1, s] = (buf[1, s].astype(f32) + tmp[...]).astype(bf16)
            send_away_mid(s).start()

            @pl.when(s >= LAG)
            def _():
                relay_home(s - LAG)

    def hidden_step(s, c, j):
        tmp[...] = dot(hid[j], wh[1, c])
        own[s] = dot(hid[j], wh[0, c]).astype(bf16)
        push(s)

    def upstream_step(s, slot, j):
        tmp[...] = dot(up[j], wg[slot, 1], LAST)
        own[s] = dot(up[j], wg[slot, 0], LAST).astype(bf16)
        push(s)

    def wait_grad_weight(fetch):
        for side in range(2):
            load_grad_weight(side, fetch).wait()

    def next_grad_weight(fetch):
        for side in range(2):
            load_grad_weight(side, fetch).start()

    load_hidden.wait()
    for side in range(2):
        for which in range(2):
            load_key_value(side, which).wait()

    def near_hidden(i):
        @pl.when(i == 1)
        def _():
            gather(0, 0).wait_recv()

        @pl.when(i == 2)
        def _():
            for c in range(chunks):
                for side in range(2):
                    load_weight(side, c).wait()

        c = jnp.where(i < 2, chunks, lax.div(i, 2) - 1)
        hidden_step(i, c, lax.rem(i, 2))

    loop(2 + 2 * chunks, near_hidden)

    load_upstream.wait()
    gather(0, 1).wait_recv()
    gather(0, 2).start()
    gather(1, 0).wait_recv()

    def near_upstream(i):
        fetch = lax.div(i, 2)
        j = lax.rem(i, 2)

        @pl.when(j == 0)
        def _():
            wait_grad_weight(fetch)

        upstream_step(2 + 2 * chunks + i, lax.rem(fetch, 2), j)

        @pl.when(j == 1)
        def _():
            next_grad_weight(fetch + 2)

    loop(2 * chunks, near_upstream)

    gather(1, 1).wait_recv()
    gather(1, 2).start()
    gather(0, 2).wait_recv()
    gather(1, 2).wait_recv()

    def low_copy(slot, target_slot, target):
        return copy(
            low_sent.at[slot], low_got.at[target_slot], low_send.at[slot], low_recv.at[target_slot],
            "width", target,
        )

    def low_terms(j):
        low_own[j, : 3 * rank] = dot(down[...], hid[j], LAST)
        low_own[j, 3 * rank :] = dot(output_up[...], up[j], LAST)
        acc[j] = jnp.zeros(acc.shape[1:], f32)

    loop(4, low_terms)
    rank_sum[...] = jnp.zeros_like(rank_sum)
    query_acc[...] = jnp.zeros_like(query_acc)
    key_value_acc[...] = jnp.zeros_like(key_value_acc)

    @pl.when(is_end)
    def _():
        low_sent[0] = low_own[...].astype(bf16)
        low_copy(0, 1, inner).start()

    @pl.when(is_mid)
    def _():
        low_copy(0, 1, inner).wait_recv()
        low_own[...] += low_got[1].astype(f32)
        low_sent[0] = low_own[...].astype(bf16)
        low_copy(0, 0, inner).start()

    def far_steps(i):
        c = jnp.where(i < 2, chunks, lax.div(i, 2) - 1)
        j = 2 + lax.rem(i, 2)
        first = 2 + 4 * chunks
        s = first + jnp.where(i < 2, i, 2 * i - 2)

        @pl.when((i == 4) & is_mid)
        def _():
            low_copy(1, 0, outward).wait_recv()
            got = low_got[0].astype(f32)
            low_sent[1] = (low_own[...] - low_got[1].astype(f32) + got).astype(bf16)
            low_copy(1, 0, outward).start()
            low[...] = (low_own[...] + got).astype(bf16)

        hidden_step(s, c, j)

        @pl.when(i >= 2)
        def _():
            fetch = chunks + c

            @pl.when(j == 2)
            def _():
                wait_grad_weight(fetch)

            upstream_step(s + 1, lax.rem(fetch, 2), j)

            @pl.when((j == 3) & (fetch + 2 < 2 * chunks))
            def _():
                next_grad_weight(fetch + 2)

    loop(2 + 2 * chunks, far_steps)

    @pl.when(is_mid)
    def _():
        loop(pieces, relay_home, pieces - LAG)

    def piece_of(kind, c, j):
        near = (0, 2, 2 + 2 * chunks)[kind] + 2 * c + j
        first = 2 + 4 * chunks
        far = first + j - 2 if kind == 0 else first + kind + 1 + 4 * c + 2 * (j - 2)
        return near if j < 2 else far

    even = lax.broadcasted_iota(jnp.int32, (rows, HEAD_DIM), 1) % 2 == 0

    def turned(values, start, direction):
        following = pltpu.roll(values, HEAD_DIM - 1, 1)
        preceding = pltpu.roll(values, 1, 1)
        partner = jnp.where(even, -following, preceding)
        at = pl.ds(start, rows)
        return values * cosine[at, :] + direction * partner * sine[at, :]

    def back_home(p):
        return copy(back.at[0, p], back.at[0, p], back_send.at[0, p], back_recv.at[0, p], "width", inner)

    def back_across(p):
        return copy(back.at[0, p], back.at[1, p], back_send.at[0, p], back_recv.at[1, p], "width", inner)

    def back_out(p):
        return copy(back.at[1, p], back.at[1, p], back_send.at[1, p], back_recv.at[1, p], "width", outward)

    def misc_copy(slot, target_slot, target):
        return copy(
            misc.at[slot], misc.at[target_slot], misc_send.at[slot], misc_recv.at[target_slot],
            "width", target,
        )

    outer_core = copy(outer, outer_got.at[0], outer_send.at[0], outer_recv.at[0], "ffn", core_peer)
    outer_chip = copy(outer_pair, outer_got.at[1], outer_send.at[1], outer_recv.at[1], "ffn", chip_peer)

    @pl.when(is_end)
    def _():
        low_copy(0, 0, inner).wait_recv()
        low[...] = (low_own[...] + low_got[0].astype(f32)).astype(bf16)
        outer[...] = jnp.zeros_like(outer)
        key_grad[...] = jnp.zeros_like(key_grad)
        value_grad[...] = jnp.zeros_like(value_grad)
        head_col = pl.multiple_of(half * HEAD_DIM, HEAD_DIM)
        key_map = key_value_up[0, :, pl.ds(head_col, HEAD_DIM)]
        value_map = key_value_up[1, :, pl.ds(head_col, HEAD_DIM)]
        for j in range(4):
            s = piece_of(0, 0, j)
            arrived(0, s)
            start = pl.multiple_of(other_index(f, j) * rows, rows)
            total = buf[0, s].astype(f32) + own[s].astype(f32)
            key_sum = total[:, :HEAD_DIM] + adapter_scale * dot(low[j, rank : 2 * rank], key_map, FIRST)
            value_sum = total[:, HEAD_DIM:] + adapter_scale * dot(
                low[j, 2 * rank : 3 * rank], value_map, FIRST
            )
            key_state[pl.ds(start, rows), :] = turned(key_sum, start, 1.0).astype(bf16)
            value_state[pl.ds(start, rows), :] = value_sum.astype(bf16)

        def heads(c):
            for j in range(4):
                for kind in (1, 2):
                    arrived(0, piece_of(kind, c, j))

            def one_head(head):
                lane = pl.multiple_of(head * HEAD_DIM, HEAD_DIM)
                lanes = pl.ds(lane, HEAD_DIM)
                first = pl.multiple_of(half * side_cols + c * cols + lane, HEAD_DIM)
                query_map = query_up[:, pl.ds(first, HEAD_DIM)]
                grad_map = output_down[:, pl.ds(first, HEAD_DIM)]
                map_grad = jnp.zeros((rank, HEAD_DIM), f32)
                for block in range(BLOCKS):
                    start, stop = block * rows, (block + 1) * rows
                    j = other_index(f, block)
                    near = j < 2
                    base = 2 + 4 * chunks
                    s_q = jnp.where(near, 2 + 2 * c + j, base + 2 + 4 * c + 2 * (j - 2))
                    s_g = jnp.where(near, 2 + 2 * chunks + 2 * c + j, base + 3 + 4 * c + 2 * (j - 2))
                    query_sum = buf[0, s_q, :, lanes].astype(f32) + own[s_q, :, lanes].astype(f32)
                    query_sum += adapter_scale * dot(low[j, :rank], query_map, FIRST)
                    query = turned(query_sum, start, 1.0).astype(bf16)
                    grad_sum = buf[0, s_g, :, lanes].astype(f32) + own[s_g, :, lanes].astype(f32)
                    out_rank = low[j, 3 * rank :]
                    grad = (grad_sum + adapter_scale * dot(out_rank, grad_map, FIRST)).astype(bf16)
                    key_part = key_state[:stop, :]
                    value_part = value_state[:stop, :]
                    scores = dot(query, key_part, LAST) * score_scale
                    row = start + lax.broadcasted_iota(jnp.int32, (rows, stop), 0)
                    column = lax.broadcasted_iota(jnp.int32, (rows, stop), 1)
                    scores = jnp.where(row >= column, scores, -jnp.inf)
                    shifted = jnp.exp(scores - jnp.max(scores, axis=1, keepdims=True))
                    probs = shifted * (1.0 / jnp.sum(shifted, axis=1, keepdims=True))
                    weights = probs.astype(bf16)
                    attended = dot(weights, value_part).astype(bf16)
                    outer[j] += dot(grad_map, attended, LAST)
                    map_grad += dot(out_rank, attended)
                    prob_grad = dot(grad, value_part, LAST)
                    delta = jnp.sum(
                        grad.astype(f32) * attended.astype(f32), axis=1, keepdims=True
                    )
                    score_grad = (probs * ((prob_grad - delta) * score_scale)).astype(bf16)
                    p = 4 * c + lax.rem(j + 2, 4)
                    back[0, p, :, lanes] = turned(dot(score_grad, key_part), start, -1.0).astype(bf16)
                    key_grad[:stop, :] += dot(score_grad, query, FIRST)
                    value_grad[:stop, :] += dot(weights, grad, FIRST)
                misc[0, 4 + c, :, lanes] = adapter_scale * map_grad

            loop(CHUNK_HEADS, one_head)
            for k in range(4):
                back_home(4 * c + k).start()

        loop(chunks, heads)
        outer_core.start()
        outer_core.wait_recv()
        for j in range(4):
            outer_pair[j] = outer[j] + outer_got[0, j + 1 - 2 * (j % 2)]
        outer_chip.start()
        for k in range(4):
            j = (k + 2) % 4
            start = pl.multiple_of(other_index(f, j) * rows, rows)
            key_block = turned(key_grad[pl.ds(start, rows), :], start, -1.0)
            back[0, 4 * chunks + k, :, :HEAD_DIM] = key_block.astype(bf16)
            back[0, 4 * chunks + k, :, HEAD_DIM:] = value_grad[pl.ds(start, rows), :].astype(bf16)
            back_home(4 * chunks + k).start()
        outer_chip.wait_recv()
        for j in range(4):
            misc[0, j] = outer_pair[j] + outer_got[1, (j + 2) % 4]
        misc_copy(0, 0, inner).start()

    def back_arrived(side, p):
        copy(
            back.at[side, p], back.at[side, p], back_send.at[side, p], back_recv.at[side, p],
            "width", inner,
        ).wait_recv()

    def absorb(side, p):
        c = lax.div(p, 4)
        j = lax.rem(lax.rem(p, 4) + 2, 4)
        step = min(2 * cols, width)
        for n in range(width // step):
            at = slice(n * step, (n + 1) * step)
            acc[j, :, at] += dot(back[side, p], wh[side, c, at, :], LAST)
        which = side_of(side)

        @pl.when(c < chunks)
        def _():
            column = pl.multiple_of(which * side_cols + c * cols, cols)
            rank_sum[j, :rank] += dot(query_up[:, pl.ds(column, cols)], back[side, p], LAST)
            query_acc[which * chunks + c] += dot(low[j, :rank], back[side, p])

        @pl.when(c == chunks)
        def _():
            column = pl.multiple_of(which * HEAD_DIM, HEAD_DIM)
            for i in range(2):
                values = back[side, p, :, i * HEAD_DIM : (i + 1) * HEAD_DIM]
                at = slice((i + 1) * rank, (i + 2) * rank)
                rank_sum[j, at] += dot(key_value_up[i, :, pl.ds(column, HEAD_DIM)], values, LAST)
                key_value_acc[which, i] += dot(low[j, at], values)

    def back_step(t):
        @pl.when((t < back_pieces) & is_mid)
        def _():
            back_arrived(0, t)
            back_across(t).start()

        @pl.when(t >= BACK_LAG)
        def _():
            back_arrived(1, t - BACK_LAG)

            @pl.when(is_mid)
            def _():
                back_out(t - BACK_LAG).start()

        def absorb_side(side):
            p = t - BACK_LAG * side

            @pl.when((p >= 0) & (p < back_pieces))
            def _():
                absorb(side, p)

        loop(2, absorb_side)

    def land_copy(first, count, slot, at, sem, axis, target):
        return copy(
            own.at[pl.ds(first, count)], land.at[slot, pl.ds(at, count)],
            land_send.at[sem], land_recv.at[sem], axis, target,
        )

    far_pair = land_copy(0, tiles, 1, 0, 0, "ffn", core_peer)
    near_pair = land_copy(tiles, tiles, 0, 0, 1, "ffn", core_peer)
    parts = 4
    per_part = tiles // parts
    chip_parts = [
        land_copy(2 * tiles + n * per_part, per_part, 2, n * per_part, 2 + n, "ffn", chip_peer)
        for n in range(parts)
    ]

    @pl.when(is_mid)
    def _():
        loop(pieces, lambda s: send_home(s).wait_send())

    loop(back_pieces - 2 + BACK_LAG, back_step)
    for n in range(tiles):
        own[n] = acc[3, :, n * cols : (n + 1) * cols].astype(bf16)
    far_pair.start()
    loop(back_pieces + BACK_LAG, back_step, back_pieces - 2 + BACK_LAG)
    far_pair.wait_recv()
    for n in range(tiles):
        pair = acc[2, :, n * cols : (n + 1) * cols] + land[1, n].astype(f32)
        own[2 * tiles + n] = pair.astype(bf16)
    for part in chip_parts[: parts // 2]:
        part.start()
    rank_core = copy(rank_sum, rank_got.at[0], rank_send.at[0], rank_recv.at[0], "ffn", core_peer)
    rank_chip = copy(rank_pair, rank_got.at[1], rank_send.at[1], rank_recv.at[1], "ffn", chip_peer)
    rank_core.start()
    for n in range(tiles):
        own[tiles + n] = acc[1, :, n * cols : (n + 1) * cols].astype(bf16)
    near_pair.start()
    rank_core.wait_recv()
    for j in range(4):
        rank_pair[j] = rank_sum[j] + rank_got[0, j + 1 - 2 * (j % 2)]
    rank_chip.start()
    for part in chip_parts[parts // 2 :]:
        part.start()

    @pl.when(is_mid)
    def _():
        misc_copy(0, 0, inner).wait_recv()
        misc_copy(0, 1, inner).start()
        misc_copy(1, 1, outward).wait_recv()
        misc_copy(1, 1, outward).start()

    @pl.when(is_end)
    def _():
        misc_copy(1, 1, inner).wait_recv()

    outer_rank = [(misc[0, j] + misc[1, j]).astype(bf16) for j in range(4)]
    for side in range(2):
        for c in range(chunks):
            column = pl.multiple_of(side_of(side) * side_cols + c * cols, cols)
            output_down_out[:, pl.ds(column, cols)] = misc[side, 4 + c]
    for c in range(2 * chunks):
        query_up_out[:, c * cols : (c + 1) * cols] = adapter_scale * query_acc[c]
    for which in range(2):
        for i in range(2):
            at = slice(which * HEAD_DIM, (which + 1) * HEAD_DIM)
            key_value_up_out[i, :, at] = adapter_scale * key_value_acc[which, i]
    total = dot(outer_rank[0], up[0])
    for j in range(1, 4):
        total += dot(outer_rank[j], up[j])
    output_up_out[...] = adapter_scale * total
    rank_chip.wait_recv()
    ranks = [(rank_pair[j] + rank_got[1, (j + 2) % 4]).astype(bf16) for j in range(4)]
    total = dot(ranks[0], hid[0])
    for j in range(1, 4):
        total += dot(ranks[j], hid[j])
    down_out[...] = adapter_scale * total
    near_pair.wait_recv()
    for n in range(tiles):
        at = slice(n * cols, (n + 1) * cols)
        acc[0, :, at] += land[0, n].astype(f32) + adapter_scale * dot(ranks[0], down[:, at], FIRST)
    for part_index, part in enumerate(chip_parts):
        part.wait_recv()
        for n in range(part_index * per_part, (part_index + 1) * per_part):
            at = slice(n * cols, (n + 1) * cols)
            hidden_out[:, at] = (acc[0, :, at] + land[2, n].astype(f32)).astype(bf16)

    for which in range(2):
        for kind in range(3):
            gather(which, kind).wait_send()
    loop(pieces, lambda s: send_away_end(s).wait_send())
    loop(back_pieces, lambda p: back_home(p).wait_send())
    low_copy(0, 0, inner).wait_send()
    misc_copy(0, 0, inner).wait_send()

    @pl.when(is_mid)
    def _():
        loop(back_pieces, lambda p: back_out(p).wait_send())
        low_copy(1, 0, outward).wait_send()
        misc_copy(1, 1, outward).wait_send()

    @pl.when(is_end)
    def _():
        outer_core.wait_send()
        outer_chip.wait_send()

    far_pair.wait_send()
    near_pair.wait_send()
    for part in chip_parts:
        part.wait_send()
    rank_core.wait_send()
    rank_chip.wait_send()


def one_kernel(
    hidden,
    upstream,
    query_frozen_weight,
    key_value_frozen_weight,
    output_frozen_weight,
    adapter_down,
    query_up_map,
    key_value_up_maps,
    output_down_map,
    output_up,
):
    bf16, f32 = jnp.bfloat16, jnp.float32
    rows, width = hidden.shape
    query_cols = query_frozen_weight.shape[1]
    cols = CHUNK_HEADS * HEAD_DIM
    chunks = query_cols // 2 // cols
    pieces = 4 + 8 * chunks
    back_pieces = 4 * chunks + 4
    tiles = width // cols
    tokens = 4 * rows
    rank = ADAPTER_RANK
    head_dims = np.arange(HEAD_DIM)
    frequency = np.exp((head_dims - head_dims % 2) * (-math.log(rope_base) / HEAD_DIM))
    angles = np.arange(tokens)[:, None] * frequency[None, :]
    cosine = jnp.asarray(np.cos(angles), f32)
    sine = jnp.asarray(np.sin(angles), f32)
    vmem = pl.BlockSpec(memory_space=pltpu.VMEM)
    hbm = pl.BlockSpec(memory_space=pl.ANY)
    dma = pltpu.SemaphoreType.DMA
    shape = jax.ShapeDtypeStruct
    outputs = pl.pallas_call(
        functools.partial(fused, 1.0 / math.sqrt(HEAD_DIM)),
        out_shape=(
            shape((rows, width), bf16),
            shape((3 * rank, width), f32),
            shape(query_up_map.shape, f32),
            shape(key_value_up_maps.shape, f32),
            shape(output_down_map.shape, f32),
            shape(output_up.shape, f32),
        ),
        in_specs=[hbm] * 5 + [vmem] * 7,
        out_specs=(vmem,) * 6,
        scratch_shapes=[
            pltpu.VMEM((4, rows, width), bf16),
            pltpu.VMEM((4, rows, width), bf16),
            pltpu.VMEM((2, chunks + 1, width, cols), bf16),
            pltpu.VMEM((2, 2, cols, width), bf16),
            pltpu.VMEM((2, pieces, rows, cols), bf16),
            pltpu.VMEM((pieces, rows, cols), bf16),
            pltpu.VMEM((2, back_pieces, rows, cols), bf16),
            pltpu.VMEM((4, rows, width), f32),
            pltpu.VMEM((3, tiles, rows, cols), bf16),
            pltpu.VMEM((rows, cols), f32),
            pltpu.VMEM((tokens, HEAD_DIM), bf16),
            pltpu.VMEM((tokens, HEAD_DIM), bf16),
            pltpu.VMEM((tokens, HEAD_DIM), f32),
            pltpu.VMEM((tokens, HEAD_DIM), f32),
            pltpu.VMEM((4, 4 * rank, rows), f32),
            pltpu.VMEM((2, 4, 4 * rank, rows), bf16),
            pltpu.VMEM((2, 4, 4 * rank, rows), bf16),
            pltpu.VMEM((4, 4 * rank, rows), bf16),
            pltpu.VMEM((4, 3 * rank, rows), f32),
            pltpu.VMEM((4, 3 * rank, rows), f32),
            pltpu.VMEM((2, 4, 3 * rank, rows), f32),
            pltpu.VMEM((4, rank, rows), f32),
            pltpu.VMEM((4, rank, rows), f32),
            pltpu.VMEM((2, 4, rank, rows), f32),
            pltpu.VMEM((2, 4 + chunks, rank, cols), f32),
            pltpu.VMEM((2 * chunks, rank, cols), f32),
            pltpu.VMEM((2, 2, rank, HEAD_DIM), f32),
            dma((2,)),
            dma((2, chunks + 2)),
            dma((2, 2)),
            dma((2, 3)),
            dma((2, 3)),
            dma((2, pieces)),
            dma((2, pieces)),
            dma((2, back_pieces)),
            dma((2, back_pieces)),
            dma((2,)),
            dma((2,)),
            dma((2,)),
            dma((2,)),
            dma((2,)),
            dma((2,)),
            dma((6,)),
            dma((6,)),
            dma((2,)),
            dma((2,)),
        ],
        compiler_params=pltpu.CompilerParams(
            collective_id=0, has_side_effects=True, vmem_limit_bytes=67_000_000
        ),
    )(
        hidden,
        upstream,
        query_frozen_weight,
        key_value_frozen_weight,
        output_frozen_weight,
        cosine,
        sine,
        adapter_down.reshape(3 * rank, width),
        query_up_map,
        key_value_up_maps,
        output_down_map,
        output_up,
    )
    return (outputs[0], outputs[1].reshape(adapter_down.shape), *outputs[2:])


def by_shape(*arrays):
    rows, width = arrays[0].shape
    cols = CHUNK_HEADS * HEAD_DIM
    fits = (
        arrays[3].shape[2] == 2 * HEAD_DIM
        and lax.axis_size("width") == 4
        and lax.axis_size("ffn") == 4
        and arrays[2].shape[1] % (2 * cols) == 0
        and rows == cols
        and width % (4 * cols) == 0
    )
    return one_kernel(*arrays) if fits else shards(*arrays)


def solution(mesh):
    placed = (
        P(("groups", "ffn"), "width"),
        P(("groups", "ffn"), "width"),
        P("width", "ffn"),
        P(None, "width", "ffn"),
        P("ffn", "width"),
        P("groups", None, "width"),
        P("groups", "ffn"),
        P("groups", None, "ffn"),
        P("groups", "ffn"),
        P("groups", "width"),
    )
    return jax.shard_map(
        by_shape,
        mesh=mesh,
        in_specs=placed,
        out_specs=(
            P(("groups", "ffn"), "width"),
            P("groups", None, "width"),
            P("groups", "ffn"),
            P("groups", None, "ffn"),
            P("groups", "ffn"),
            P("groups", "width"),
        ),
        check_vma=False,
    )
```

```python
import functools
import math

import jax
import jax.numpy as jnp
import numpy as np
from jax import lax
from jax.experimental import pallas as pl
from jax.experimental.pallas import tpu as pltpu
from jax.sharding import PartitionSpec as P

KV_HEADS = 8
HEAD_DIM = 128
ADAPTER_RANK = 16
CHUNK_HEADS = 2
BLOCKS = 4
LAG = 3
MESH = pl.DeviceIdType.MESH
LAST = (((1,), (1,)), ((), ()))
FIRST = (((0,), (0,)), ((), ()))


adapter_scale = 2.0
rope_base = 500000.0


def from_partner(array, axis, bit):
    return lax.ppermute(array, axis, [(i, i ^ 1 << bit) for i in range(lax.axis_size(axis))])


def rotate(values, positions, first_dim, direction):
    columns = values.shape[1]
    head_dims = (first_dim + jnp.arange(columns, dtype=jnp.int32)) % HEAD_DIM
    pair_dims = head_dims - head_dims % 2
    frequency = jnp.exp(pair_dims.astype(jnp.float32) * (-math.log(rope_base) / HEAD_DIM))
    angles = positions.astype(jnp.float32)[:, None] * frequency[None, :]
    is_even = head_dims % 2 == 0
    following = jnp.roll(values, -1, axis=1)
    preceding = jnp.roll(values, 1, axis=1)
    partner = jnp.where(is_even[None, :], -following, preceding)
    return values * jnp.cos(angles) + direction * partner * jnp.sin(angles)


def contract_last(left_side, right_side):
    return lax.dot_general(
        left_side, right_side, (((1,), (1,)), ((), ())), preferred_element_type=jnp.float32
    )


def contract_leading(left_side, right_side):
    return lax.dot_general(
        left_side, right_side, (((0,), (0,)), ((), ())), preferred_element_type=jnp.float32
    )


def shards(
    hidden,
    upstream,
    query_frozen_weight,
    key_value_frozen_weight,
    output_frozen_weight,
    adapter_down,
    query_up_map,
    key_value_up_maps,
    output_down_map,
    output_up,
):
    ffn_count = lax.axis_size("ffn")
    width_count = lax.axis_size("width")
    ffn_index = lax.axis_index("ffn")
    width_index = lax.axis_index("width")
    hidden_rows_full, upstream_gradient_full = (
        lax.all_gather(hidden, "ffn", axis=0, tiled=True),
        lax.all_gather(upstream, "ffn", axis=0, tiled=True),
    )
    token_count = hidden_rows_full.shape[0]
    query_rows = token_count // width_count
    query_cols = query_frozen_weight.shape[1]
    key_cols = key_value_frozen_weight.shape[2]
    row_start = width_index * query_rows
    positions = jnp.arange(token_count, dtype=jnp.int32)
    row_positions = row_start + jnp.arange(query_rows, dtype=jnp.int32)
    query_offset = ffn_index * query_cols
    key_offset = ffn_index * key_cols
    score_scale = 1.0 / math.sqrt(HEAD_DIM)
    down_flattened = adapter_down.reshape(3 * ADAPTER_RANK, adapter_down.shape[2])
    paired = ffn_count > KV_HEADS
    parity = ffn_index % 2
    rank_terms = contract_last(hidden_rows_full, down_flattened)
    upstream_terms = contract_last(upstream_gradient_full, output_up)
    rank_sum, upstream_sum = lax.psum((rank_terms, upstream_terms), "width")
    reduced_hidden = rank_sum.astype(jnp.bfloat16)
    output_reduced = upstream_sum.astype(jnp.bfloat16)
    low_rows = lax.dynamic_slice_in_dim(reduced_hidden, row_start, query_rows, 0)
    output_token_rows = lax.dynamic_slice_in_dim(output_reduced, row_start, query_rows, 0)
    query_part = jnp.dot(hidden_rows_full, query_frozen_weight, preferred_element_type=jnp.float32)
    query_gradient_summed = lax.psum_scatter(
        query_part.astype(jnp.bfloat16), "width", scatter_dimension=0, tiled=True
    ).astype(jnp.float32)
    query_projected = query_gradient_summed + adapter_scale * jnp.dot(
        low_rows[:, :ADAPTER_RANK], query_up_map, preferred_element_type=jnp.float32
    )
    query_states = rotate(query_projected, row_positions, query_offset, 1.0).astype(jnp.bfloat16)
    key_part = jnp.dot(
        hidden_rows_full, key_value_frozen_weight[0], preferred_element_type=jnp.float32
    )
    value_part = jnp.dot(
        hidden_rows_full, key_value_frozen_weight[1], preferred_element_type=jnp.float32
    )
    key_gradient_summed, value_gradient_summed = (
        lax.psum_scatter(
            key_part.astype(jnp.bfloat16), "width", scatter_dimension=0, tiled=True
        ).astype(jnp.float32),
        lax.psum_scatter(
            value_part.astype(jnp.bfloat16), "width", scatter_dimension=0, tiled=True
        ).astype(jnp.float32),
    )
    key_projected = key_gradient_summed + adapter_scale * jnp.dot(
        low_rows[:, ADAPTER_RANK : 2 * ADAPTER_RANK],
        key_value_up_maps[0],
        preferred_element_type=jnp.float32,
    )
    value_projected = value_gradient_summed + adapter_scale * jnp.dot(
        low_rows[:, 2 * ADAPTER_RANK :], key_value_up_maps[1], preferred_element_type=jnp.float32
    )
    key_block = rotate(key_projected, row_positions, key_offset, 1.0).astype(jnp.bfloat16)
    value_block = value_projected.astype(jnp.bfloat16)
    key_states, value_state_rows = (
        lax.all_gather(key_block, "width", axis=0, tiled=True),
        lax.all_gather(value_block, "width", axis=0, tiled=True),
    )
    if paired:
        other_key, other_value = from_partner((key_states, value_state_rows), "ffn", 0)
        key_states = jnp.where(
            parity == 0,
            jnp.concatenate([key_states, other_key], 1),
            jnp.concatenate([other_key, key_states], 1),
        )
        value_state_rows = jnp.where(
            parity == 0,
            jnp.concatenate([value_state_rows, other_value], 1),
            jnp.concatenate([other_value, value_state_rows], 1),
        )
    local_heads = query_cols // HEAD_DIM
    local_groups = key_states.shape[1] // HEAD_DIM
    group_size = local_heads // local_groups
    query_four = query_states.reshape(query_rows, local_groups, group_size, HEAD_DIM)
    key_three = key_states.reshape(token_count, local_groups, HEAD_DIM)
    value_three = value_state_rows.reshape(token_count, local_groups, HEAD_DIM)
    causal = row_positions[:, None] >= positions[None, :]
    scores = (
        jnp.einsum("qkgd,skd->kgqs", query_four, key_three, preferred_element_type=jnp.float32)
        * score_scale
    )
    scores = jnp.where(causal[None, None, :, :], scores, -jnp.inf)
    shifted = jnp.exp(scores - jnp.max(scores, axis=-1, keepdims=True))
    probs = shifted / jnp.sum(shifted, axis=-1, keepdims=True)
    prob_weights = probs.astype(jnp.bfloat16)
    attention_four = jnp.einsum(
        "kgqs,skd->qkgd", prob_weights, value_three, preferred_element_type=jnp.float32
    ).astype(jnp.bfloat16)
    attention_output = attention_four.reshape(query_rows, query_cols)
    out_part = contract_last(upstream_gradient_full, output_frozen_weight)
    output_gradient_summed = lax.psum_scatter(
        out_part.astype(jnp.bfloat16), "width", scatter_dimension=0, tiled=True
    ).astype(jnp.float32)
    attention_output_gradient = (
        output_gradient_summed
        + adapter_scale
        * jnp.dot(output_token_rows, output_down_map, preferred_element_type=jnp.float32)
    ).astype(jnp.bfloat16)
    grad_four = attention_output_gradient.reshape(query_rows, local_groups, group_size, HEAD_DIM)
    prob_grad = jnp.einsum(
        "qkgd,skd->kgqs", grad_four, value_three, preferred_element_type=jnp.float32
    )
    delta = jnp.einsum(
        "qkgd,qkgd->kgq", grad_four, attention_four, preferred_element_type=jnp.float32
    )
    score_grad = (probs * (prob_grad - delta[:, :, :, None]) * score_scale).astype(jnp.bfloat16)
    query_rot_grad = jnp.einsum(
        "kgqs,skd->qkgd", score_grad, key_three, preferred_element_type=jnp.float32
    ).reshape(query_rows, query_cols)
    key_part_grad = jnp.einsum(
        "kgqs,qkgd->skd", score_grad, query_four, preferred_element_type=jnp.float32
    ).reshape(token_count, local_groups * HEAD_DIM)
    value_part_grad = jnp.einsum(
        "kgqs,qkgd->skd", prob_weights, grad_four, preferred_element_type=jnp.float32
    ).reshape(token_count, local_groups * HEAD_DIM)
    query_block_grad = rotate(query_rot_grad, row_positions, query_offset, -1.0).astype(
        jnp.bfloat16
    )

    def own_half(values):
        return lax.dynamic_slice_in_dim(values, parity * key_cols, key_cols, 1)

    def other_half(values):
        return lax.dynamic_slice_in_dim(values, (1 - parity) * key_cols, key_cols, 1)

    key_total, value_total = lax.psum((key_part_grad, value_part_grad), "width")
    if paired:
        sent_key, sent_value = from_partner(
            (other_half(key_total), other_half(value_total)), "ffn", 0
        )
        key_total = own_half(key_total) + sent_key
        value_total = own_half(value_total) + sent_value
    key_rows_gradient = rotate(key_total, positions, key_offset, -1.0).astype(jnp.bfloat16)
    value_rows_gradient = value_total.astype(jnp.bfloat16)
    query_rows_gradient = lax.all_gather(query_block_grad, "width", axis=0, tiled=True)
    input_part = (
        contract_last(query_rows_gradient, query_frozen_weight)
        + contract_last(key_rows_gradient, key_value_frozen_weight[0])
        + contract_last(value_rows_gradient, key_value_frozen_weight[1])
    )
    rank_grad_terms = jnp.concatenate(
        [
            contract_last(query_rows_gradient, query_up_map),
            contract_last(key_rows_gradient, key_value_up_maps[0]),
            contract_last(value_rows_gradient, key_value_up_maps[1]),
        ],
        axis=1,
    )
    rank_gradient = lax.psum(rank_grad_terms, "ffn").astype(jnp.bfloat16)
    input_sum = lax.psum_scatter(
        input_part.astype(jnp.bfloat16), "ffn", scatter_dimension=0, tiled=True
    ).astype(jnp.float32)
    own_rows = token_count // ffn_count
    rank_gradient_token_rows = lax.dynamic_slice_in_dim(
        rank_gradient, ffn_index * own_rows, own_rows, 0
    )
    hidden_gradient = (
        input_sum
        + adapter_scale
        * jnp.dot(rank_gradient_token_rows, down_flattened, preferred_element_type=jnp.float32)
    ).astype(jnp.bfloat16)
    down_map_gradient = (adapter_scale * contract_leading(rank_gradient, hidden_rows_full)).reshape(
        adapter_down.shape
    )
    query_up_map_gradient = adapter_scale * contract_leading(
        reduced_hidden[:, :ADAPTER_RANK], query_rows_gradient
    )
    key_value_up_maps_gradient = adapter_scale * jnp.stack(
        [
            contract_leading(reduced_hidden[:, ADAPTER_RANK : 2 * ADAPTER_RANK], key_rows_gradient),
            contract_leading(reduced_hidden[:, 2 * ADAPTER_RANK :], value_rows_gradient),
        ]
    )
    outer_terms = contract_last(attention_output, output_down_map)
    outer_rows = lax.psum(outer_terms, "ffn").astype(jnp.bfloat16)
    outer_product_rank = lax.all_gather(outer_rows, "width", axis=0, tiled=True)
    output_down_map_gradient = adapter_scale * lax.psum(
        contract_leading(output_token_rows, attention_output), "width"
    )
    output_up_map_gradient = adapter_scale * contract_leading(
        outer_product_rank, upstream_gradient_full
    )
    return (
        hidden_gradient,
        down_map_gradient,
        query_up_map_gradient,
        key_value_up_maps_gradient,
        output_down_map_gradient,
        output_up_map_gradient,
    )


def dot(left, right, dims=None):
    if dims is None:
        return jnp.dot(left, right, preferred_element_type=jnp.float32)
    return lax.dot_general(left, right, dims, preferred_element_type=jnp.float32)


def other_index(a, b):
    low = lax.rem(lax.rem(a, 2) + lax.rem(b, 2), 2)
    high = lax.rem(lax.div(a, 2) + lax.div(b, 2), 2)
    return 2 * high + low


def fused(
    score_scale,
    hidden_in, upstream_in, query_weight, key_value_weight, output_weight,
    *refs,
):
    small_in, results, small, staged = refs[:7], refs[7:13], refs[13:20], refs[20:26]
    (
        hid, up, wh, wg, buf, own, back, acc, land, tmp, key_state, value_state, key_grad, value_grad,
        low_own, low_sent, low_got, low, rank_sum, rank_pair, rank_got, rank_far, outer, outer_pair,
        outer_got, misc, query_acc, key_value_acc,
        load_sem, weight_sem, grad_sem, gather_send, gather_recv, send_sem, recv_sem, back_send,
        back_recv, low_send, low_recv, misc_send, misc_recv, outer_send, outer_recv, land_send,
        land_recv, rank_send, rank_recv, small_sem, result_sem,
    ) = refs[26:]
    cosine, sine, down, query_up, key_value_up, output_down, output_up = small
    hidden_out, down_out, query_up_out, key_value_up_out, output_down_out, output_up_out = staged
    bf16, f32 = jnp.bfloat16, jnp.float32
    rows, width = hidden_in.shape
    cols = CHUNK_HEADS * HEAD_DIM
    chunks = wh.shape[1] - 1
    side_cols = chunks * cols
    rank = ADAPTER_RANK
    last = chunks - 1
    near_end = 2 + 4 * last
    far_end = 2 * near_end
    pieces = far_end + 8
    far_back = 4 + 2 * chunks
    back_pieces = 4 + 4 * chunks
    tiles = width // cols
    f = lax.axis_index("ffn")
    z = lax.axis_index("width")
    half = lax.div(z, 2)
    ahead = 1 - 2 * half
    inner = z + ahead
    outward = z - ahead
    is_end = (z == 0) | (z == 3)
    is_mid = (z == 1) | (z == 2)
    core_peer = f + 1 - 2 * lax.rem(f, 2)
    chip_peer = lax.rem(f + 2, 4)

    def copy(src, dst, send, recv, axis, target):
        return pltpu.make_async_remote_copy(
            src_ref=src, dst_ref=dst, send_sem=send, recv_sem=recv,
            device_id={axis: target}, device_id_type=MESH,
        )

    def side_of(side):
        return half + side * (1 - 2 * half)

    def loop(count, step, start=0):
        def run(i, carry):
            step(i)
            return carry
        lax.fori_loop(start, count, run, 0)

    load_hidden = pltpu.make_async_copy(hidden_in, hid.at[0], load_sem.at[0])
    load_upstream = pltpu.make_async_copy(upstream_in, up.at[0], load_sem.at[1])

    def load_weight(side, c):
        start = pl.multiple_of(side_of(side) * side_cols + c * cols, cols)
        return pltpu.make_async_copy(
            query_weight.at[:, pl.ds(start, cols)], wh.at[side, c], weight_sem.at[side, c]
        )

    def load_key_value(side, which):
        start = pl.multiple_of(side_of(side) * HEAD_DIM, HEAD_DIM)
        return pltpu.make_async_copy(
            key_value_weight.at[which, :, pl.ds(start, HEAD_DIM)],
            wh.at[side, chunks, :, pl.ds(which * HEAD_DIM, HEAD_DIM)],
            weight_sem.at[side, chunks + which],
        )

    def load_grad_weight(side, fetch):
        c = jnp.where(fetch == 2 * last, last, lax.rem(fetch, last))
        start = pl.multiple_of(side_of(side) * side_cols + c * cols, cols)
        slot = lax.rem(fetch, 2)
        return pltpu.make_async_copy(
            output_weight.at[pl.ds(start, cols), :], wg.at[slot, side], grad_sem.at[slot, side]
        )

    load_small = [
        pltpu.make_async_copy(source, target, small_sem.at[n])
        for n, (source, target) in enumerate(zip(small_in, small))
    ]
    barrier = pltpu.get_barrier_semaphore()
    pl.semaphore_signal(barrier, inc=1, device_id={"ffn": core_peer}, device_id_type=MESH)
    pl.semaphore_signal(barrier, inc=1, device_id={"ffn": chip_peer}, device_id_type=MESH)
    pl.semaphore_signal(barrier, inc=1, device_id={"width": inner}, device_id_type=MESH)

    @pl.when(is_mid)
    def _():
        pl.semaphore_signal(barrier, inc=1, device_id={"width": outward}, device_id_type=MESH)

    load_hidden.start()
    for side in range(2):
        for which in range(2):
            load_key_value(side, which).start()

    @pl.when(is_mid)
    def _():
        pl.semaphore_wait(barrier, 4)

    @pl.when(is_end)
    def _():
        pl.semaphore_wait(barrier, 3)

    def gather(which, kind):
        source, full = ((hidden_in, hid), (upstream_in, up))[which]
        sems = gather_send.at[which, kind], gather_recv.at[which, kind]
        if kind == 0:
            return copy(source, full.at[1], *sems, "ffn", core_peer)
        if kind == 1:
            return copy(source, full.at[2], *sems, "ffn", chip_peer)
        return copy(full.at[2], full.at[3], *sems, "ffn", core_peer)

    for which in range(2):
        gather(which, 1).start()
        gather(which, 0).start()
    for c in range(chunks):
        for side in range(2):
            load_weight(side, c).start()
    load_upstream.start()
    for fetch in range(2):
        for side in range(2):
            load_grad_weight(side, fetch).start()
    for load in load_small:
        load.start()

    def send_away_end(s):
        return copy(buf.at[1, s], buf.at[1, s], send_sem.at[1, s], recv_sem.at[1, s], "width", inner)

    def send_away_mid(s):
        return copy(buf.at[1, s], buf.at[0, s], send_sem.at[1, s], recv_sem.at[0, s], "width", inner)

    def send_home(s):
        return copy(buf.at[0, s], buf.at[0, s], send_sem.at[0, s], recv_sem.at[0, s], "width", outward)

    def arrived(side, s):
        copy(
            buf.at[side, s], buf.at[side, s], send_sem.at[side, s], recv_sem.at[side, s], "width", inner
        ).wait_recv()

    def relay_home(s):
        arrived(0, s)
        buf[0, s] = (buf[0, s].astype(f32) + own[s].astype(f32)).astype(bf16)
        send_home(s).start()

    def push(s):
        @pl.when(is_end)
        def _():
            buf[1, s] = tmp[...].astype(bf16)
            send_away_end(s).start()

        @pl.when(is_mid)
        def _():
            arrived(1, s)
            buf[1, s] = (buf[1, s].astype(f32) + tmp[...]).astype(bf16)
            send_away_mid(s).start()

            @pl.when(s >= LAG)
            def _():
                relay_home(s - LAG)

    def hidden_step(s, c, j):
        tmp[...] = dot(hid[j], wh[1, c])
        own[s] = dot(hid[j], wh[0, c]).astype(bf16)
        push(s)

    def upstream_step(s, slot, j):
        tmp[...] = dot(up[j], wg[slot, 1], LAST)
        own[s] = dot(up[j], wg[slot, 0], LAST).astype(bf16)
        push(s)

    def wait_grad_weight(fetch):
        for side in range(2):
            load_grad_weight(side, fetch).wait()

    def next_grad_weight(fetch):
        for side in range(2):
            load_grad_weight(side, fetch).start()

    load_hidden.wait()
    for side in range(2):
        for which in range(2):
            load_key_value(side, which).wait()

    def low_copy(slot, target_slot, target):
        return copy(
            low_sent.at[slot], low_got.at[target_slot], low_send.at[slot], low_recv.at[target_slot],
            "width", target,
        )

    def low_terms(j):
        low_own[j, : 3 * rank] = dot(down[...], hid[j], LAST)
        low_own[j, 3 * rank :] = dot(output_up[...], up[j], LAST)

    def forward_step(s):
        late = s >= near_end
        r = s - jnp.where(late, near_end, 0) - 2
        key_value = r < 0
        full = jnp.maximum(r, 0)
        tail = s - far_end
        in_last = tail >= 0
        tail = jnp.maximum(tail, 0)
        quarter = lax.rem(full, 4)
        c = jnp.where(key_value, chunks, jnp.where(in_last, last, lax.div(full, 4)))
        grad = jnp.where(in_last, lax.rem(tail, 2), lax.div(quarter, 2))
        is_grad = (grad == 1) & (r >= 0)
        j = jnp.where(key_value, r + 2, lax.rem(quarter, 2)) + jnp.where(late, 2, 0)
        j = jnp.where(in_last, lax.rem(lax.div(tail, 2) + 2, 4), j)
        fetch = jnp.where(in_last, 2 * last, c + jnp.where(late, last, 0))

        @pl.when(s == 1)
        def _():
            gather(0, 0).wait_recv()

        @pl.when(s == 2)
        def _():
            for n in range(chunks):
                for side in range(2):
                    load_weight(side, n).wait()

        @pl.when(s == 4)
        def _():
            load_upstream.wait()

        @pl.when(s == 5)
        def _():
            gather(1, 0).wait_recv()

        @pl.when(s == 8)
        def _():
            for load in load_small:
                load.wait()

        @pl.when(s == near_end)
        def _():
            gather(0, 1).wait_recv()
            gather(0, 2).start()

        @pl.when(s == near_end + 1)
        def _():
            gather(0, 2).wait_recv()

        @pl.when(s == near_end + 4)
        def _():
            gather(1, 1).wait_recv()
            gather(1, 2).start()

        @pl.when(s == near_end + 5)
        def _():
            gather(1, 2).wait_recv()

        near_low = (s == 8) | (s == 9)
        far_low = (s == near_end + 4) | (s == near_end + 5)

        @pl.when(near_low | far_low)
        def _():
            low_terms(jnp.where(s < near_end, s - 8, s - near_end - 2))

        @pl.when((s >= 10) & (s < 14))
        def _():
            acc[s - 10] = jnp.zeros(acc.shape[1:], f32)

        @pl.when((s == near_end + 6) & is_end)
        def _():
            low_sent[0] = low_own[...].astype(bf16)
            low_copy(0, 1, inner).start()

        @pl.when((s == near_end + 6) & is_mid)
        def _():
            low_copy(0, 1, inner).wait_recv()
            low_sent[0] = (low_own[...] + low_got[1].astype(f32)).astype(bf16)
            low_copy(0, 0, inner).start()

        @pl.when((s == near_end + 6 + LAG) & is_mid)
        def _():
            low_copy(1, 0, outward).wait_recv()
            total = low_own[...] + low_got[0].astype(f32)
            low_sent[1] = total.astype(bf16)
            low_copy(1, 0, outward).start()
            low[...] = (total + low_got[1].astype(f32)).astype(bf16)

        @pl.when(~is_grad)
        def _():
            hidden_step(s, c, j)

        @pl.when(is_grad)
        def _():
            first = jnp.where(in_last, s == far_end + 1, lax.rem(j, 2) == 0)

            @pl.when(first)
            def _():
                wait_grad_weight(fetch)

            upstream_step(s, lax.rem(fetch, 2), j)

            @pl.when((lax.rem(j, 2) == 1) & (fetch + 2 <= 2 * last) & (s < far_end))
            def _():
                next_grad_weight(fetch + 2)

    rank_sum[...] = jnp.zeros_like(rank_sum)
    query_acc[...] = jnp.zeros_like(query_acc)
    key_value_acc[...] = jnp.zeros_like(key_value_acc)
    loop(pieces, forward_step)

    def piece_of(kind, c, j):
        if kind == 0:
            return j if j < 2 else near_end + j - 2
        spread = jnp.where(j < 2, 2 + j, near_end + j) + 4 * c + 2 * (kind - 1)
        return jnp.where(c == last, far_end + 2 * lax.rem(j + 2, 4) + kind - 1, spread)

    def back_index(c, j):
        if isinstance(c, int):
            if c == 0:
                return (j + 2) % 4
            return 2 * c + j if j >= 2 else 2 + 2 * chunks + 2 * c + j
        later = jnp.where(j >= 2, 2 * c + j, 2 + 2 * chunks + 2 * c + j)
        return jnp.where(c == 0, lax.rem(j + 2, 4), later)

    even = lax.broadcasted_iota(jnp.int32, (rows, HEAD_DIM), 1) % 2 == 0

    def turned(values, start, direction):
        following = pltpu.roll(values, HEAD_DIM - 1, 1)
        preceding = pltpu.roll(values, 1, 1)
        partner = jnp.where(even, -following, preceding)
        at = pl.ds(start, rows)
        return values * cosine[at, :] + direction * partner * sine[at, :]

    def back_home(p):
        return copy(back.at[0, p], back.at[0, p], back_send.at[0, p], back_recv.at[0, p], "width", inner)

    def back_across(p):
        return copy(back.at[0, p], back.at[1, p], back_send.at[0, p], back_recv.at[1, p], "width", inner)

    def back_out(p):
        return copy(back.at[1, p], back.at[1, p], back_send.at[1, p], back_recv.at[1, p], "width", outward)

    def misc_copy(slot, target_slot, target):
        return copy(
            misc.at[slot], misc.at[target_slot], misc_send.at[slot], misc_recv.at[target_slot],
            "width", target,
        )

    def back_arrived(side, p):
        copy(
            back.at[side, p], back.at[side, p], back_send.at[side, p], back_recv.at[side, p],
            "width", inner,
        ).wait_recv()

    def drain(i):
        back_arrived(0, i)
        back_across(i).start()
        relay_home(pieces - LAG + i)

    @pl.when(is_mid)
    def _():
        loop(LAG, drain)

    outer_core = copy(outer, outer_got.at[0], outer_send.at[0], outer_recv.at[0], "ffn", core_peer)
    outer_chip = copy(outer_pair, outer_got.at[1], outer_send.at[1], outer_recv.at[1], "ffn", chip_peer)

    @pl.when(is_end)
    def _():
        low_copy(0, 0, inner).wait_recv()
        low[...] = (low_own[...] + low_got[0].astype(f32)).astype(bf16)
        outer[...] = jnp.zeros_like(outer)
        misc[0] = jnp.zeros(misc.shape[1:], f32)
        key_grad[...] = jnp.zeros_like(key_grad)
        value_grad[...] = jnp.zeros_like(value_grad)
        head_col = pl.multiple_of(half * HEAD_DIM, HEAD_DIM)
        key_map = key_value_up[0, :, pl.ds(head_col, HEAD_DIM)]
        value_map = key_value_up[1, :, pl.ds(head_col, HEAD_DIM)]
        for j in range(4):
            s = piece_of(0, 0, j)
            arrived(0, s)
            start = pl.multiple_of(other_index(f, j) * rows, rows)
            total = buf[0, s].astype(f32) + own[s].astype(f32)
            key_sum = total[:, :HEAD_DIM] + adapter_scale * dot(low[j, rank : 2 * rank], key_map, FIRST)
            value_sum = total[:, HEAD_DIM:] + adapter_scale * dot(
                low[j, 2 * rank : 3 * rank], value_map, FIRST
            )
            key_state[pl.ds(start, rows), :] = turned(key_sum, start, 1.0).astype(bf16)
            value_state[pl.ds(start, rows), :] = value_sum.astype(bf16)

        def block_of_head(c, j, head, block):
            lane = pl.multiple_of(head * HEAD_DIM, HEAD_DIM)
            lanes = pl.ds(lane, HEAD_DIM)
            first = pl.multiple_of(half * side_cols + c * cols + lane, HEAD_DIM)
            query_map = query_up[:, pl.ds(first, HEAD_DIM)]
            grad_map = output_down[:, pl.ds(first, HEAD_DIM)]
            start, stop = block * rows, (block + 1) * rows
            s_q, s_g = piece_of(1, c, j), piece_of(2, c, j)
            query_sum = buf[0, s_q, :, lanes].astype(f32) + own[s_q, :, lanes].astype(f32)
            query_sum += adapter_scale * dot(low[j, :rank], query_map, FIRST)
            query = turned(query_sum, start, 1.0).astype(bf16)
            grad_sum = buf[0, s_g, :, lanes].astype(f32) + own[s_g, :, lanes].astype(f32)
            out_rank = low[j, 3 * rank :]
            grad = (grad_sum + adapter_scale * dot(out_rank, grad_map, FIRST)).astype(bf16)
            key_part = key_state[:stop, :]
            value_part = value_state[:stop, :]
            scores = dot(query, key_part, LAST) * score_scale
            row = start + lax.broadcasted_iota(jnp.int32, (rows, stop), 0)
            column = lax.broadcasted_iota(jnp.int32, (rows, stop), 1)
            scores = jnp.where(row >= column, scores, -jnp.inf)
            shifted = jnp.exp(scores - jnp.max(scores, axis=1, keepdims=True))
            probs = shifted * (1.0 / jnp.sum(shifted, axis=1, keepdims=True))
            weights = probs.astype(bf16)
            attended = dot(weights, value_part).astype(bf16)
            outer[j] += dot(grad_map, attended, LAST)
            misc[0, 4 + c, :, lanes] += adapter_scale * dot(out_rank, attended)
            prob_grad = dot(grad, value_part, LAST)
            delta = jnp.sum(grad.astype(f32) * attended.astype(f32), axis=1, keepdims=True)
            score_grad = (probs * ((prob_grad - delta) * score_scale)).astype(bf16)
            turned_grad = turned(dot(score_grad, key_part), start, -1.0)
            back[0, back_index(c, j), :, lanes] = turned_grad.astype(bf16)
            key_grad[:stop, :] += dot(score_grad, query, FIRST)
            value_grad[:stop, :] += dot(weights, grad, FIRST)

        def attend(i):
            c = lax.div(i, 4)
            j = lax.rem(i + 2, 4)
            arrived(0, piece_of(1, c, j))
            arrived(0, piece_of(2, c, j))
            here = other_index(f, j)

            def one_head(head):
                for block in range(BLOCKS):
                    pl.when(here == block)(
                        functools.partial(block_of_head, c, j, head, block)
                    )

            loop(CHUNK_HEADS, one_head)

            @pl.when((c == 0) | (j >= 2))
            def _():
                back_home(back_index(c, j)).start()

        loop(4 * chunks, attend)
        outer_core.start()

        def send_key_value(j):
            p = back_index(chunks, j)
            start = pl.multiple_of(other_index(f, j) * rows, rows)
            key_block = turned(key_grad[pl.ds(start, rows), :], start, -1.0)
            back[0, p, :, :HEAD_DIM] = key_block.astype(bf16)
            back[0, p, :, HEAD_DIM:] = value_grad[pl.ds(start, rows), :].astype(bf16)
            back_home(p).start()

        send_key_value(2)
        send_key_value(3)
        for c in range(1, chunks):
            for j in range(2):
                back_home(back_index(c, j)).start()
        outer_core.wait_recv()
        for j in range(4):
            outer_pair[j] = outer[j] + outer_got[0, j + 1 - 2 * (j % 2)]
        outer_chip.start()
        outer_chip.wait_recv()
        for j in range(4):
            misc[0, j] = outer_pair[j] + outer_got[1, (j + 2) % 4]
        misc_copy(0, 0, inner).start()
        send_key_value(0)
        send_key_value(1)

    def absorb(side, p):
        late = p >= far_back
        r = jnp.maximum(p - jnp.where(late, far_back, 4), 0)
        c = jnp.where(p < 4, 0, 1 + lax.div(r, 2))
        j = jnp.where(p < 4, lax.rem(p + 2, 4), lax.rem(r, 2) + jnp.where(late, 0, 2))
        step = min(2 * cols, width)
        for n in range(width // step):
            at = slice(n * step, (n + 1) * step)
            acc[j, :, at] += dot(back[side, p], wh[side, c, at, :], LAST)
        which = side_of(side)

        @pl.when(c < chunks)
        def _():
            column = pl.multiple_of(which * side_cols + c * cols, cols)
            rank_sum[j, :rank] += dot(query_up[:, pl.ds(column, cols)], back[side, p], LAST)
            query_acc[which * chunks + c] += dot(low[j, :rank], back[side, p])

        @pl.when(c == chunks)
        def _():
            column = pl.multiple_of(which * HEAD_DIM, HEAD_DIM)
            for i in range(2):
                values = back[side, p, :, i * HEAD_DIM : (i + 1) * HEAD_DIM]
                at = slice((i + 1) * rank, (i + 2) * rank)
                rank_sum[j, at] += dot(key_value_up[i, :, pl.ds(column, HEAD_DIM)], values, LAST)
                key_value_acc[which, i] += dot(low[j, at], values)

    def land_copy(first, count, slot, at, sem, axis, target):
        return copy(
            own.at[pl.ds(first, count)], land.at[slot, pl.ds(at, count)],
            land_send.at[sem], land_recv.at[sem], axis, target,
        )

    far_pair = land_copy(0, tiles, 1, 0, 0, "ffn", core_peer)
    near_pair = land_copy(tiles, tiles, 0, 0, 1, "ffn", core_peer)
    parts = 4
    per_part = tiles // parts
    chip_parts = [
        land_copy(2 * tiles + n * per_part, per_part, 2, n * per_part, 2 + n, "ffn", chip_peer)
        for n in range(parts)
    ]

    def back_step(t):
        @pl.when((t == back_pieces - 2 - LAG) & is_mid)
        def _():
            misc_copy(0, 0, inner).wait_recv()
            misc_copy(0, 1, inner).start()

        @pl.when((t + LAG < back_pieces) & is_mid)
        def _():
            back_arrived(0, t + LAG)
            back_across(t + LAG).start()

        @pl.when(t == back_pieces - 2)
        def _():
            misc_copy(1, 1, inner).wait_recv()

        @pl.when((t == back_pieces - 2) & is_mid)
        def _():
            misc_copy(1, 1, outward).start()

        back_arrived(1, t)

        @pl.when(is_mid)
        def _():
            back_out(t).start()

        loop(2, lambda side: absorb(side, t))

        @pl.when(t == far_back - 1)
        def _():
            for n in range(tiles):
                own[n] = acc[3, :, n * cols : (n + 1) * cols].astype(bf16)
            far_pair.start()

        @pl.when(t == far_back + 1)
        def _():
            far_pair.wait_recv()
            for n in range(tiles):
                pair = acc[2, :, n * cols : (n + 1) * cols] + land[1, n].astype(f32)
                own[2 * tiles + n] = pair.astype(bf16)
            for part in chip_parts:
                part.start()

    loop(back_pieces, back_step)
    rank_core = copy(rank_sum, rank_got, rank_send.at[0], rank_recv.at[0], "ffn", core_peer)
    rank_chip = copy(rank_pair, rank_far, rank_send.at[1], rank_recv.at[1], "ffn", chip_peer)
    rank_core.start()
    for n in range(tiles):
        own[tiles + n] = acc[1, :, n * cols : (n + 1) * cols].astype(bf16)
    near_pair.start()
    rank_core.wait_recv()
    for j in range(4):
        rank_pair[j] = (rank_sum[j] + rank_got[j + 1 - 2 * (j % 2)]).astype(bf16)
    rank_chip.start()

    def put(n):
        return pltpu.make_async_copy(staged[n], results[n], result_sem.at[n])

    outer_rank = [(misc[0, j] + misc[1, j]).astype(bf16) for j in range(4)]
    for side in range(2):
        for c in range(chunks):
            column = pl.multiple_of(side_of(side) * side_cols + c * cols, cols)
            output_down_out[:, pl.ds(column, cols)] = misc[side, 4 + c]
    for c in range(2 * chunks):
        query_up_out[:, c * cols : (c + 1) * cols] = adapter_scale * query_acc[c]
    for which in range(2):
        for i in range(2):
            at = slice(which * HEAD_DIM, (which + 1) * HEAD_DIM)
            key_value_up_out[i, :, at] = adapter_scale * key_value_acc[which, i]
    total = dot(outer_rank[0], up[0])
    for j in range(1, 4):
        total += dot(outer_rank[j], up[j])
    output_up_out[...] = adapter_scale * total
    for n in range(2, 6):
        put(n).start()
    near_pair.wait_recv()
    for n in range(tiles):
        at = slice(n * cols, (n + 1) * cols)
        acc[0, :, at] += land[0, n].astype(f32)
    rank_chip.wait_recv()
    ranks = [
        (rank_pair[j].astype(f32) + rank_far[(j + 2) % 4].astype(f32)).astype(bf16) for j in range(4)
    ]
    total = dot(ranks[0], hid[0])
    for j in range(1, 4):
        total += dot(ranks[j], hid[j])
    down_out[...] = adapter_scale * total
    put(1).start()
    part_cols = per_part * cols
    put_parts = [
        pltpu.make_async_copy(
            hidden_out.at[:, pl.ds(n * part_cols, part_cols)],
            results[0].at[:, pl.ds(n * part_cols, part_cols)],
            result_sem.at[6 + n],
        )
        for n in range(parts)
    ]
    for part_index, part in enumerate(chip_parts):
        part.wait_recv()
        for n in range(part_index * per_part, (part_index + 1) * per_part):
            at = slice(n * cols, (n + 1) * cols)
            adapter = adapter_scale * dot(ranks[0], down[:, at], FIRST)
            hidden_out[:, at] = (acc[0, :, at] + land[2, n].astype(f32) + adapter).astype(bf16)
        put_parts[part_index].start()

    for which in range(2):
        for kind in range(3):
            gather(which, kind).wait_send()
    loop(pieces, lambda s: send_away_end(s).wait_send())
    loop(back_pieces, lambda p: back_home(p).wait_send())
    low_copy(0, 0, inner).wait_send()
    misc_copy(0, 0, inner).wait_send()

    @pl.when(is_mid)
    def _():
        loop(pieces, lambda s: send_home(s).wait_send())
        loop(back_pieces, lambda p: back_out(p).wait_send())
        low_copy(1, 0, outward).wait_send()
        misc_copy(1, 1, outward).wait_send()

    @pl.when(is_end)
    def _():
        outer_core.wait_send()
        outer_chip.wait_send()

    far_pair.wait_send()
    near_pair.wait_send()
    for part in chip_parts:
        part.wait_send()
    rank_core.wait_send()
    rank_chip.wait_send()
    for n in range(1, 6):
        put(n).wait()
    for part in put_parts:
        part.wait()


def pass_on(*refs):
    count = (len(refs) - 2) // 3
    sources, results, held = refs[:count], refs[count : 2 * count], refs[2 * count : 3 * count]
    in_sem, out_sem = refs[3 * count :]
    fetch = [pltpu.make_async_copy(s, h, in_sem.at[n]) for n, (s, h) in enumerate(zip(sources, held))]
    store = [pltpu.make_async_copy(h, r, out_sem.at[n]) for n, (h, r) in enumerate(zip(held, results))]
    for copy in fetch:
        copy.start()
    for arrived, copy in zip(fetch, store):
        arrived.wait()
        copy.start()
    for copy in store:
        copy.wait()


def one_kernel(
    hidden,
    upstream,
    query_frozen_weight,
    key_value_frozen_weight,
    output_frozen_weight,
    adapter_down,
    query_up_map,
    key_value_up_maps,
    output_down_map,
    output_up,
):
    bf16, f32 = jnp.bfloat16, jnp.float32
    rows, width = hidden.shape
    query_cols = query_frozen_weight.shape[1]
    cols = CHUNK_HEADS * HEAD_DIM
    chunks = query_cols // 2 // cols
    pieces = 4 + 8 * chunks
    back_pieces = 4 * chunks + 4
    tiles = width // cols
    tokens = 4 * rows
    rank = ADAPTER_RANK
    head_dims = np.arange(HEAD_DIM)
    frequency = np.exp((head_dims - head_dims % 2) * (-math.log(rope_base) / HEAD_DIM))
    angles = np.arange(tokens)[:, None] * frequency[None, :]
    cosine = jnp.asarray(np.cos(angles), f32)
    sine = jnp.asarray(np.sin(angles), f32)
    hbm = pl.BlockSpec(memory_space=pl.ANY)
    dma = pltpu.SemaphoreType.DMA
    shape = jax.ShapeDtypeStruct
    results = (
        shape((rows, width), bf16),
        shape((3 * rank, width), f32),
        shape(query_up_map.shape, f32),
        shape(key_value_up_maps.shape, f32),
        shape(output_down_map.shape, f32),
        shape(output_up.shape, f32),
    )
    held = [pltpu.VMEM(result.shape, result.dtype) for result in results]
    small = (
        cosine,
        sine,
        adapter_down.reshape(3 * rank, width),
        query_up_map,
        key_value_up_maps,
        output_down_map,
        output_up,
    )
    outputs = pl.pallas_call(
        functools.partial(fused, 1.0 / math.sqrt(HEAD_DIM)),
        out_shape=results,
        in_specs=[hbm] * 12,
        out_specs=(hbm,) * 6,
        scratch_shapes=[
            *[pltpu.VMEM(array.shape, array.dtype) for array in small],
            *held,
            pltpu.VMEM((4, rows, width), bf16),
            pltpu.VMEM((4, rows, width), bf16),
            pltpu.VMEM((2, chunks + 1, width, cols), bf16),
            pltpu.VMEM((2, 2, cols, width), bf16),
            pltpu.VMEM((2, pieces, rows, cols), bf16),
            pltpu.VMEM((pieces, rows, cols), bf16),
            pltpu.VMEM((2, back_pieces, rows, cols), bf16),
            pltpu.VMEM((4, rows, width), f32),
            pltpu.VMEM((3, tiles, rows, cols), bf16),
            pltpu.VMEM((rows, cols), f32),
            pltpu.VMEM((tokens, HEAD_DIM), bf16),
            pltpu.VMEM((tokens, HEAD_DIM), bf16),
            pltpu.VMEM((tokens, HEAD_DIM), f32),
            pltpu.VMEM((tokens, HEAD_DIM), f32),
            pltpu.VMEM((4, 4 * rank, rows), f32),
            pltpu.VMEM((2, 4, 4 * rank, rows), bf16),
            pltpu.VMEM((2, 4, 4 * rank, rows), bf16),
            pltpu.VMEM((4, 4 * rank, rows), bf16),
            pltpu.VMEM((4, 3 * rank, rows), f32),
            pltpu.VMEM((4, 3 * rank, rows), bf16),
            pltpu.VMEM((4, 3 * rank, rows), f32),
            pltpu.VMEM((4, 3 * rank, rows), bf16),
            pltpu.VMEM((4, rank, rows), f32),
            pltpu.VMEM((4, rank, rows), f32),
            pltpu.VMEM((2, 4, rank, rows), f32),
            pltpu.VMEM((2, 4 + chunks, rank, cols), f32),
            pltpu.VMEM((2 * chunks, rank, cols), f32),
            pltpu.VMEM((2, 2, rank, HEAD_DIM), f32),
            dma((2,)),
            dma((2, chunks + 2)),
            dma((2, 2)),
            dma((2, 3)),
            dma((2, 3)),
            dma((2, pieces)),
            dma((2, pieces)),
            dma((2, back_pieces)),
            dma((2, back_pieces)),
            dma((2,)),
            dma((2,)),
            dma((2,)),
            dma((2,)),
            dma((2,)),
            dma((2,)),
            dma((6,)),
            dma((6,)),
            dma((2,)),
            dma((2,)),
            dma((7,)),
            dma((10,)),
        ],
        compiler_params=pltpu.CompilerParams(
            collective_id=0, has_side_effects=True, vmem_limit_bytes=67_000_000
        ),
    )(
        hidden,
        upstream,
        query_frozen_weight,
        key_value_frozen_weight,
        output_frozen_weight,
        *small,
    )
    outputs = pl.pallas_call(
        pass_on,
        out_shape=results,
        in_specs=[hbm] * 6,
        out_specs=(hbm,) * 6,
        scratch_shapes=[*held, dma((6,)), dma((6,))],
    )(*outputs)
    return (outputs[0], outputs[1].reshape(adapter_down.shape), *outputs[2:])


def by_shape(*arrays):
    rows, width = arrays[0].shape
    cols = CHUNK_HEADS * HEAD_DIM
    fits = (
        arrays[3].shape[2] == 2 * HEAD_DIM
        and lax.axis_size("width") == 4
        and lax.axis_size("ffn") == 4
        and arrays[2].shape[1] % (2 * cols) == 0
        and arrays[2].shape[1] >= 6 * cols
        and rows == cols
        and width % (4 * cols) == 0
    )
    return one_kernel(*arrays) if fits else shards(*arrays)


def solution(mesh):
    placed = (
        P(("groups", "ffn"), "width"),
        P(("groups", "ffn"), "width"),
        P("width", "ffn"),
        P(None, "width", "ffn"),
        P("ffn", "width"),
        P("groups", None, "width"),
        P("groups", "ffn"),
        P("groups", None, "ffn"),
        P("groups", "ffn"),
        P("groups", "width"),
    )
    return jax.shard_map(
        by_shape,
        mesh=mesh,
        in_specs=placed,
        out_specs=(
            P(("groups", "ffn"), "width"),
            P("groups", None, "width"),
            P("groups", "ffn"),
            P("groups", None, "ffn"),
            P("groups", "ffn"),
            P("groups", "width"),
        ),
        check_vma=False,
    )
```

```python
import functools
import math

import jax
import jax.numpy as jnp
import numpy as np
from jax import lax
from jax.experimental import pallas as pl
from jax.experimental.pallas import tpu as pltpu
from jax.sharding import PartitionSpec as P

KV_HEADS = 8
HEAD_DIM = 128
ADAPTER_RANK = 16
CHUNK_HEADS = 2
BLOCKS = 4
LAG = 4
MESH = pl.DeviceIdType.MESH
LAST = (((1,), (1,)), ((), ()))
FIRST = (((0,), (0,)), ((), ()))


adapter_scale = 2.0
rope_base = 500000.0


def from_partner(array, axis, bit):
    return lax.ppermute(array, axis, [(i, i ^ 1 << bit) for i in range(lax.axis_size(axis))])


def rotate(values, positions, first_dim, direction):
    columns = values.shape[1]
    head_dims = (first_dim + jnp.arange(columns, dtype=jnp.int32)) % HEAD_DIM
    pair_dims = head_dims - head_dims % 2
    frequency = jnp.exp(pair_dims.astype(jnp.float32) * (-math.log(rope_base) / HEAD_DIM))
    angles = positions.astype(jnp.float32)[:, None] * frequency[None, :]
    is_even = head_dims % 2 == 0
    following = jnp.roll(values, -1, axis=1)
    preceding = jnp.roll(values, 1, axis=1)
    partner = jnp.where(is_even[None, :], -following, preceding)
    return values * jnp.cos(angles) + direction * partner * jnp.sin(angles)


def contract_last(left_side, right_side):
    return lax.dot_general(
        left_side, right_side, (((1,), (1,)), ((), ())), preferred_element_type=jnp.float32
    )


def contract_leading(left_side, right_side):
    return lax.dot_general(
        left_side, right_side, (((0,), (0,)), ((), ())), preferred_element_type=jnp.float32
    )


def shards(
    hidden,
    upstream,
    query_frozen_weight,
    key_value_frozen_weight,
    output_frozen_weight,
    adapter_down,
    query_up_map,
    key_value_up_maps,
    output_down_map,
    output_up,
):
    ffn_count = lax.axis_size("ffn")
    width_count = lax.axis_size("width")
    ffn_index = lax.axis_index("ffn")
    width_index = lax.axis_index("width")
    hidden_rows_full, upstream_gradient_full = (
        lax.all_gather(hidden, "ffn", axis=0, tiled=True),
        lax.all_gather(upstream, "ffn", axis=0, tiled=True),
    )
    token_count = hidden_rows_full.shape[0]
    query_rows = token_count // width_count
    query_cols = query_frozen_weight.shape[1]
    key_cols = key_value_frozen_weight.shape[2]
    row_start = width_index * query_rows
    positions = jnp.arange(token_count, dtype=jnp.int32)
    row_positions = row_start + jnp.arange(query_rows, dtype=jnp.int32)
    query_offset = ffn_index * query_cols
    key_offset = ffn_index * key_cols
    score_scale = 1.0 / math.sqrt(HEAD_DIM)
    down_flattened = adapter_down.reshape(3 * ADAPTER_RANK, adapter_down.shape[2])
    paired = ffn_count > KV_HEADS
    parity = ffn_index % 2
    rank_terms = contract_last(hidden_rows_full, down_flattened)
    upstream_terms = contract_last(upstream_gradient_full, output_up)
    rank_sum, upstream_sum = lax.psum((rank_terms, upstream_terms), "width")
    reduced_hidden = rank_sum.astype(jnp.bfloat16)
    output_reduced = upstream_sum.astype(jnp.bfloat16)
    low_rows = lax.dynamic_slice_in_dim(reduced_hidden, row_start, query_rows, 0)
    output_token_rows = lax.dynamic_slice_in_dim(output_reduced, row_start, query_rows, 0)
    query_part = jnp.dot(hidden_rows_full, query_frozen_weight, preferred_element_type=jnp.float32)
    query_gradient_summed = lax.psum_scatter(
        query_part.astype(jnp.bfloat16), "width", scatter_dimension=0, tiled=True
    ).astype(jnp.float32)
    query_projected = query_gradient_summed + adapter_scale * jnp.dot(
        low_rows[:, :ADAPTER_RANK], query_up_map, preferred_element_type=jnp.float32
    )
    query_states = rotate(query_projected, row_positions, query_offset, 1.0).astype(jnp.bfloat16)
    key_part = jnp.dot(
        hidden_rows_full, key_value_frozen_weight[0], preferred_element_type=jnp.float32
    )
    value_part = jnp.dot(
        hidden_rows_full, key_value_frozen_weight[1], preferred_element_type=jnp.float32
    )
    key_gradient_summed, value_gradient_summed = (
        lax.psum_scatter(
            key_part.astype(jnp.bfloat16), "width", scatter_dimension=0, tiled=True
        ).astype(jnp.float32),
        lax.psum_scatter(
            value_part.astype(jnp.bfloat16), "width", scatter_dimension=0, tiled=True
        ).astype(jnp.float32),
    )
    key_projected = key_gradient_summed + adapter_scale * jnp.dot(
        low_rows[:, ADAPTER_RANK : 2 * ADAPTER_RANK],
        key_value_up_maps[0],
        preferred_element_type=jnp.float32,
    )
    value_projected = value_gradient_summed + adapter_scale * jnp.dot(
        low_rows[:, 2 * ADAPTER_RANK :], key_value_up_maps[1], preferred_element_type=jnp.float32
    )
    key_block = rotate(key_projected, row_positions, key_offset, 1.0).astype(jnp.bfloat16)
    value_block = value_projected.astype(jnp.bfloat16)
    key_states, value_state_rows = (
        lax.all_gather(key_block, "width", axis=0, tiled=True),
        lax.all_gather(value_block, "width", axis=0, tiled=True),
    )
    if paired:
        other_key, other_value = from_partner((key_states, value_state_rows), "ffn", 0)
        key_states = jnp.where(
            parity == 0,
            jnp.concatenate([key_states, other_key], 1),
            jnp.concatenate([other_key, key_states], 1),
        )
        value_state_rows = jnp.where(
            parity == 0,
            jnp.concatenate([value_state_rows, other_value], 1),
            jnp.concatenate([other_value, value_state_rows], 1),
        )
    local_heads = query_cols // HEAD_DIM
    local_groups = key_states.shape[1] // HEAD_DIM
    group_size = local_heads // local_groups
    query_four = query_states.reshape(query_rows, local_groups, group_size, HEAD_DIM)
    key_three = key_states.reshape(token_count, local_groups, HEAD_DIM)
    value_three = value_state_rows.reshape(token_count, local_groups, HEAD_DIM)
    causal = row_positions[:, None] >= positions[None, :]
    scores = (
        jnp.einsum("qkgd,skd->kgqs", query_four, key_three, preferred_element_type=jnp.float32)
        * score_scale
    )
    scores = jnp.where(causal[None, None, :, :], scores, -jnp.inf)
    shifted = jnp.exp(scores - jnp.max(scores, axis=-1, keepdims=True))
    probs = shifted / jnp.sum(shifted, axis=-1, keepdims=True)
    prob_weights = probs.astype(jnp.bfloat16)
    attention_four = jnp.einsum(
        "kgqs,skd->qkgd", prob_weights, value_three, preferred_element_type=jnp.float32
    ).astype(jnp.bfloat16)
    attention_output = attention_four.reshape(query_rows, query_cols)
    out_part = contract_last(upstream_gradient_full, output_frozen_weight)
    output_gradient_summed = lax.psum_scatter(
        out_part.astype(jnp.bfloat16), "width", scatter_dimension=0, tiled=True
    ).astype(jnp.float32)
    attention_output_gradient = (
        output_gradient_summed
        + adapter_scale
        * jnp.dot(output_token_rows, output_down_map, preferred_element_type=jnp.float32)
    ).astype(jnp.bfloat16)
    grad_four = attention_output_gradient.reshape(query_rows, local_groups, group_size, HEAD_DIM)
    prob_grad = jnp.einsum(
        "qkgd,skd->kgqs", grad_four, value_three, preferred_element_type=jnp.float32
    )
    delta = jnp.einsum(
        "qkgd,qkgd->kgq", grad_four, attention_four, preferred_element_type=jnp.float32
    )
    score_grad = (probs * (prob_grad - delta[:, :, :, None]) * score_scale).astype(jnp.bfloat16)
    query_rot_grad = jnp.einsum(
        "kgqs,skd->qkgd", score_grad, key_three, preferred_element_type=jnp.float32
    ).reshape(query_rows, query_cols)
    key_part_grad = jnp.einsum(
        "kgqs,qkgd->skd", score_grad, query_four, preferred_element_type=jnp.float32
    ).reshape(token_count, local_groups * HEAD_DIM)
    value_part_grad = jnp.einsum(
        "kgqs,qkgd->skd", prob_weights, grad_four, preferred_element_type=jnp.float32
    ).reshape(token_count, local_groups * HEAD_DIM)
    query_block_grad = rotate(query_rot_grad, row_positions, query_offset, -1.0).astype(
        jnp.bfloat16
    )

    def own_half(values):
        return lax.dynamic_slice_in_dim(values, parity * key_cols, key_cols, 1)

    def other_half(values):
        return lax.dynamic_slice_in_dim(values, (1 - parity) * key_cols, key_cols, 1)

    key_total, value_total = lax.psum((key_part_grad, value_part_grad), "width")
    if paired:
        sent_key, sent_value = from_partner(
            (other_half(key_total), other_half(value_total)), "ffn", 0
        )
        key_total = own_half(key_total) + sent_key
        value_total = own_half(value_total) + sent_value
    key_rows_gradient = rotate(key_total, positions, key_offset, -1.0).astype(jnp.bfloat16)
    value_rows_gradient = value_total.astype(jnp.bfloat16)
    query_rows_gradient = lax.all_gather(query_block_grad, "width", axis=0, tiled=True)
    input_part = (
        contract_last(query_rows_gradient, query_frozen_weight)
        + contract_last(key_rows_gradient, key_value_frozen_weight[0])
        + contract_last(value_rows_gradient, key_value_frozen_weight[1])
    )
    rank_grad_terms = jnp.concatenate(
        [
            contract_last(query_rows_gradient, query_up_map),
            contract_last(key_rows_gradient, key_value_up_maps[0]),
            contract_last(value_rows_gradient, key_value_up_maps[1]),
        ],
        axis=1,
    )
    rank_gradient = lax.psum(rank_grad_terms, "ffn").astype(jnp.bfloat16)
    input_sum = lax.psum_scatter(
        input_part.astype(jnp.bfloat16), "ffn", scatter_dimension=0, tiled=True
    ).astype(jnp.float32)
    own_rows = token_count // ffn_count
    rank_gradient_token_rows = lax.dynamic_slice_in_dim(
        rank_gradient, ffn_index * own_rows, own_rows, 0
    )
    hidden_gradient = (
        input_sum
        + adapter_scale
        * jnp.dot(rank_gradient_token_rows, down_flattened, preferred_element_type=jnp.float32)
    ).astype(jnp.bfloat16)
    down_map_gradient = (adapter_scale * contract_leading(rank_gradient, hidden_rows_full)).reshape(
        adapter_down.shape
    )
    query_up_map_gradient = adapter_scale * contract_leading(
        reduced_hidden[:, :ADAPTER_RANK], query_rows_gradient
    )
    key_value_up_maps_gradient = adapter_scale * jnp.stack(
        [
            contract_leading(reduced_hidden[:, ADAPTER_RANK : 2 * ADAPTER_RANK], key_rows_gradient),
            contract_leading(reduced_hidden[:, 2 * ADAPTER_RANK :], value_rows_gradient),
        ]
    )
    outer_terms = contract_last(attention_output, output_down_map)
    outer_rows = lax.psum(outer_terms, "ffn").astype(jnp.bfloat16)
    outer_product_rank = lax.all_gather(outer_rows, "width", axis=0, tiled=True)
    output_down_map_gradient = adapter_scale * lax.psum(
        contract_leading(output_token_rows, attention_output), "width"
    )
    output_up_map_gradient = adapter_scale * contract_leading(
        outer_product_rank, upstream_gradient_full
    )
    return (
        hidden_gradient,
        down_map_gradient,
        query_up_map_gradient,
        key_value_up_maps_gradient,
        output_down_map_gradient,
        output_up_map_gradient,
    )


def dot(left, right, dims=None):
    if dims is None:
        return jnp.dot(left, right, preferred_element_type=jnp.float32)
    return lax.dot_general(left, right, dims, preferred_element_type=jnp.float32)


def other_index(a, b):
    low = lax.rem(lax.rem(a, 2) + lax.rem(b, 2), 2)
    high = lax.rem(lax.div(a, 2) + lax.div(b, 2), 2)
    return 2 * high + low


def block_at(k):
    return jnp.where(k < 2, 3 - k, k - 2)


def place_of(j):
    return jnp.where(j < 2, j + 2, 3 - j)


def fused(
    score_scale,
    hidden_in, upstream_in, query_weight, key_value_weight, output_weight,
    *refs,
):
    small_in, results, small, staged = refs[:7], refs[7:13], refs[13:20], refs[20:26]
    (
        hid, up, wh, wg, buf, own, back, acc, land, tmp, key_state, value_state, key_grad, value_grad,
        low_own, low_sent, low_got, low, rank_sum, rank_pair, rank_got, rank_far, outer, outer_pair,
        outer_got, misc, passed, query_acc, key_value_acc,
        load_sem, weight_sem, grad_sem, gather_send, gather_recv, send_sem, recv_sem, back_send,
        back_recv, low_send, low_recv, misc_send, misc_recv, outer_send, outer_recv, land_send,
        land_recv, rank_send, rank_recv, small_sem, result_sem,
    ) = refs[26:]
    cosine, sine, down, query_up, key_value_up, output_down, output_up = small
    hidden_out, down_out, query_up_out, key_value_up_out, output_down_out, output_up_out = staged
    bf16, f32 = jnp.bfloat16, jnp.float32
    rows, width = hidden_in.shape
    cols = CHUNK_HEADS * HEAD_DIM
    chunks = wh.shape[1] - 1
    side_cols = chunks * cols
    rank = ADAPTER_RANK
    last = chunks - 1
    near_end = 2 + 4 * last
    far_end = 2 * near_end
    pieces = far_end + 8
    far_back = 4 + 2 * chunks
    back_pieces = 4 + 4 * chunks
    tiles = width // cols
    half_rows = rows // 2
    f = lax.axis_index("ffn")
    z = lax.axis_index("width")
    half = lax.div(z, 2)
    ahead = 1 - 2 * half
    inner = z + ahead
    outward = z - ahead
    is_end = (z == 0) | (z == 3)
    is_mid = (z == 1) | (z == 2)
    core_peer = f + 1 - 2 * lax.rem(f, 2)
    chip_peer = lax.rem(f + 2, 4)

    def copy(src, dst, send, recv, axis, target):
        return pltpu.make_async_remote_copy(
            src_ref=src, dst_ref=dst, send_sem=send, recv_sem=recv,
            device_id={axis: target}, device_id_type=MESH,
        )

    def side_of(side):
        return half + side * (1 - 2 * half)

    def loop(count, step, start=0):
        def run(i, carry):
            step(i)
            return carry
        lax.fori_loop(start, count, run, 0)

    load_hidden = pltpu.make_async_copy(hidden_in, hid.at[0], load_sem.at[0])
    load_upstream = pltpu.make_async_copy(upstream_in, up.at[0], load_sem.at[1])

    def load_weight(side, c):
        start = pl.multiple_of(side_of(side) * side_cols + c * cols, cols)
        return pltpu.make_async_copy(
            query_weight.at[:, pl.ds(start, cols)], wh.at[side, c], weight_sem.at[side, c]
        )

    def load_key_value(side, which):
        start = pl.multiple_of(side_of(side) * HEAD_DIM, HEAD_DIM)
        return pltpu.make_async_copy(
            key_value_weight.at[which, :, pl.ds(start, HEAD_DIM)],
            wh.at[side, chunks, :, pl.ds(which * HEAD_DIM, HEAD_DIM)],
            weight_sem.at[side, chunks + which],
        )

    def load_grad_weight(side, fetch):
        c = jnp.where(fetch == 2 * last, last, lax.rem(fetch, last))
        start = pl.multiple_of(side_of(side) * side_cols + c * cols, cols)
        slot = lax.rem(fetch, 2)
        return pltpu.make_async_copy(
            output_weight.at[pl.ds(start, cols), :], wg.at[slot, side], grad_sem.at[slot, side]
        )

    load_small = [
        pltpu.make_async_copy(source, target, small_sem.at[n])
        for n, (source, target) in enumerate(zip(small_in, small))
    ]
    barrier = pltpu.get_barrier_semaphore()
    pl.semaphore_signal(barrier, inc=1, device_id={"ffn": core_peer}, device_id_type=MESH)
    pl.semaphore_signal(barrier, inc=1, device_id={"ffn": chip_peer}, device_id_type=MESH)
    pl.semaphore_signal(barrier, inc=1, device_id={"width": inner}, device_id_type=MESH)

    @pl.when(is_mid)
    def _():
        pl.semaphore_signal(barrier, inc=1, device_id={"width": outward}, device_id_type=MESH)

    load_hidden.start()
    for side in range(2):
        for which in range(2):
            load_key_value(side, which).start()

    @pl.when(is_mid)
    def _():
        pl.semaphore_wait(barrier, 4)

    @pl.when(is_end)
    def _():
        pl.semaphore_wait(barrier, 3)

    def gather(which, kind):
        source, full = ((hidden_in, hid), (upstream_in, up))[which]
        sems = gather_send.at[which, kind], gather_recv.at[which, kind]
        if kind == 0:
            return copy(source, full.at[1], *sems, "ffn", core_peer)
        if kind == 1:
            return copy(source, full.at[2], *sems, "ffn", chip_peer)
        return copy(full.at[2], full.at[3], *sems, "ffn", core_peer)

    for which in range(2):
        gather(which, 1).start()
        gather(which, 0).start()
    for c in range(chunks):
        for side in range(2):
            load_weight(side, c).start()
    load_upstream.start()
    for fetch in range(2):
        for side in range(2):
            load_grad_weight(side, fetch).start()
    for load in load_small:
        load.start()

    def half_of(ref, side, u):
        start = pl.multiple_of(lax.rem(u, 2) * half_rows, half_rows)
        return ref.at[side, lax.div(u, 2), pl.ds(start, half_rows)]

    def send_away_end(u):
        part = half_of(buf, 1, u)
        return copy(part, part, send_sem.at[1], recv_sem.at[1, u], "width", inner)

    def send_away_mid(u):
        return copy(
            half_of(buf, 1, u), half_of(buf, 0, u), send_sem.at[1], recv_sem.at[0, u], "width", inner
        )

    def send_home(u):
        part = half_of(buf, 0, u)
        return copy(part, part, send_sem.at[0], recv_sem.at[0, u], "width", outward)

    def arrived(side, u):
        part = half_of(buf, side, u)
        copy(part, part, send_sem.at[side], recv_sem.at[side, u], "width", inner).wait_recv()

    def piece_arrived(s):
        arrived(0, 2 * s)
        arrived(0, 2 * s + 1)

    def relay_home(u):
        s = lax.div(u, 2)
        at = pl.ds(pl.multiple_of(lax.rem(u, 2) * half_rows, half_rows), half_rows)
        arrived(0, u)
        buf[0, s, at] = (buf[0, s, at].astype(f32) + own[s, at].astype(f32)).astype(bf16)
        send_home(u).start()

    def push(s):
        @pl.when(is_end)
        def _():
            buf[1, s] = tmp[...].astype(bf16)
            for h in range(2):
                send_away_end(2 * s + h).start()

        @pl.when(is_mid)
        def _():
            def one_half(h):
                u = 2 * s + h
                at = pl.ds(pl.multiple_of(h * half_rows, half_rows), half_rows)
                arrived(1, u)
                buf[1, s, at] = (buf[1, s, at].astype(f32) + tmp[at, :]).astype(bf16)
                send_away_mid(u).start()

                @pl.when(u >= LAG)
                def _():
                    relay_home(u - LAG)

            loop(2, one_half)

    def hidden_step(s, c, j):
        tmp[...] = dot(hid[j], wh[1, c])
        push(s)
        own[s] = dot(hid[j], wh[0, c]).astype(bf16)

    def upstream_step(s, slot, j):
        tmp[...] = dot(up[j], wg[slot, 1], LAST)
        push(s)
        own[s] = dot(up[j], wg[slot, 0], LAST).astype(bf16)

    def wait_grad_weight(fetch):
        for side in range(2):
            load_grad_weight(side, fetch).wait()

    def next_grad_weight(fetch):
        for side in range(2):
            load_grad_weight(side, fetch).start()

    load_hidden.wait()
    for side in range(2):
        for which in range(2):
            load_key_value(side, which).wait()

    def low_copy(slot, target_slot, target):
        return copy(
            low_sent.at[slot], low_got.at[target_slot], low_send.at[slot], low_recv.at[target_slot],
            "width", target,
        )

    def low_terms(j):
        low_own[j, : 3 * rank] = dot(down[...], hid[j], LAST)
        low_own[j, 3 * rank :] = dot(output_up[...], up[j], LAST)

    def forward_step(s):
        late = s >= near_end
        r = s - jnp.where(late, near_end, 0) - 2
        key_value = r < 0
        full = jnp.maximum(r, 0)
        tail = s - far_end
        in_last = tail >= 0
        tail = jnp.maximum(tail, 0)
        quarter = lax.rem(full, 4)
        c = jnp.where(key_value, chunks, jnp.where(in_last, last, lax.div(full, 4)))
        grad = jnp.where(in_last, lax.rem(tail, 2), lax.div(quarter, 2))
        is_grad = (grad == 1) & (r >= 0)
        j = jnp.where(key_value, r + 2, lax.rem(quarter, 2)) + jnp.where(late, 2, 0)
        j = jnp.where(in_last, block_at(lax.div(tail, 2)), j)
        fetch = jnp.where(in_last, 2 * last, c + jnp.where(late, last, 0))

        @pl.when(s == 1)
        def _():
            gather(0, 0).wait_recv()

        @pl.when(s == 2)
        def _():
            for n in range(chunks):
                for side in range(2):
                    load_weight(side, n).wait()

        @pl.when(s == 4)
        def _():
            load_upstream.wait()

        @pl.when(s == 5)
        def _():
            gather(1, 0).wait_recv()

        @pl.when(s == 8)
        def _():
            for load in load_small:
                load.wait()

        @pl.when(s == near_end)
        def _():
            gather(0, 1).wait_recv()
            gather(0, 2).start()

        @pl.when(s == near_end + 1)
        def _():
            gather(0, 2).wait_recv()

        @pl.when(s == near_end + 4)
        def _():
            gather(1, 1).wait_recv()
            gather(1, 2).start()

        @pl.when(s == near_end + 5)
        def _():
            gather(1, 2).wait_recv()

        near_low = (s == 8) | (s == 9)
        far_low = (s == near_end + 4) | (s == near_end + 5)

        @pl.when(near_low | far_low)
        def _():
            low_terms(jnp.where(s < near_end, s - 8, s - near_end - 2))

        @pl.when((s >= 10) & (s < 14))
        def _():
            acc[s - 10] = jnp.zeros(acc.shape[1:], f32)

        @pl.when((s == near_end + 6) & is_end)
        def _():
            low_sent[0] = low_own[...].astype(bf16)
            low_copy(0, 1, inner).start()

        @pl.when((s == near_end + 6) & is_mid)
        def _():
            low_copy(0, 1, inner).wait_recv()
            low_sent[0] = (low_own[...] + low_got[1].astype(f32)).astype(bf16)
            low_copy(0, 0, inner).start()

        @pl.when((s == near_end + 8) & is_mid)
        def _():
            low_copy(1, 0, outward).wait_recv()
            total = low_own[...] + low_got[0].astype(f32)
            low_sent[1] = total.astype(bf16)
            low_copy(1, 0, outward).start()
            low[...] = (total + low_got[1].astype(f32)).astype(bf16)

        @pl.when(~is_grad)
        def _():
            hidden_step(s, c, j)

        @pl.when(is_grad)
        def _():
            first = jnp.where(in_last, s == far_end + 1, lax.rem(j, 2) == 0)

            @pl.when(first)
            def _():
                wait_grad_weight(fetch)

            upstream_step(s, lax.rem(fetch, 2), j)

            @pl.when((lax.rem(j, 2) == 1) & (fetch + 2 <= 2 * last) & (s < far_end))
            def _():
                next_grad_weight(fetch + 2)

    rank_sum[...] = jnp.zeros_like(rank_sum)
    query_acc[...] = jnp.zeros_like(query_acc)
    key_value_acc[...] = jnp.zeros_like(key_value_acc)
    loop(pieces, forward_step)

    def piece_of(kind, c, j):
        if kind == 0:
            return j if j < 2 else near_end + j - 2
        spread = jnp.where(j < 2, 2 + j, near_end + j) + 4 * c + 2 * (kind - 1)
        return jnp.where(c == last, far_end + 2 * place_of(j) + kind - 1, spread)

    def back_index(c, j):
        if isinstance(c, int):
            return 2 * c + 5 - j if j >= 2 else 2 + 2 * chunks + 2 * c + j
        later = jnp.where(j >= 2, 2 * c + 5 - j, 2 + 2 * chunks + 2 * c + j)
        return jnp.where(c == 0, place_of(j), later)

    even = lax.broadcasted_iota(jnp.int32, (rows, HEAD_DIM), 1) % 2 == 0

    def turned(values, start, direction):
        following = pltpu.roll(values, HEAD_DIM - 1, 1)
        preceding = pltpu.roll(values, 1, 1)
        partner = jnp.where(even, -following, preceding)
        at = pl.ds(start, rows)
        return values * cosine[at, :] + direction * partner * sine[at, :]

    def back_home(v):
        part = half_of(back, 0, v)
        return copy(part, part, back_send.at[0], back_recv.at[0, v], "width", inner)

    def back_across(v):
        return copy(
            half_of(back, 0, v), half_of(back, 1, v), back_send.at[0], back_recv.at[1, v], "width", inner
        )

    def back_out(v):
        part = half_of(back, 1, v)
        return copy(part, part, back_send.at[1], back_recv.at[1, v], "width", outward)

    def send_back(p):
        for h in range(2):
            back_home(2 * p + h).start()

    def misc_copy(slot, target_slot, target):
        return copy(
            passed.at[slot], passed.at[target_slot], misc_send.at[slot], misc_recv.at[target_slot],
            "width", target,
        )

    def back_arrived(side, v):
        part = half_of(back, side, v)
        copy(part, part, back_send.at[side], back_recv.at[side, v], "width", inner).wait_recv()

    def drain(i):
        back_arrived(0, i)
        back_across(i).start()
        relay_home(2 * pieces - LAG + i)

    @pl.when(is_mid)
    def _():
        loop(LAG, drain)

    outer_core = copy(outer, outer_got.at[0], outer_send.at[0], outer_recv.at[0], "ffn", core_peer)
    outer_chip = copy(outer_pair, outer_got.at[1], outer_send.at[1], outer_recv.at[1], "ffn", chip_peer)

    @pl.when(is_end)
    def _():
        low_copy(0, 0, inner).wait_recv()
        low[...] = (low_own[...] + low_got[0].astype(f32)).astype(bf16)
        outer[...] = jnp.zeros_like(outer)
        misc[...] = jnp.zeros_like(misc)
        key_grad[...] = jnp.zeros_like(key_grad)
        value_grad[...] = jnp.zeros_like(value_grad)
        head_col = pl.multiple_of(half * HEAD_DIM, HEAD_DIM)
        key_map = key_value_up[0, :, pl.ds(head_col, HEAD_DIM)]
        value_map = key_value_up[1, :, pl.ds(head_col, HEAD_DIM)]
        for j in range(4):
            s = piece_of(0, 0, j)
            piece_arrived(s)
            start = pl.multiple_of(other_index(f, j) * rows, rows)
            total = buf[0, s].astype(f32) + own[s].astype(f32)
            key_sum = total[:, :HEAD_DIM] + adapter_scale * dot(low[j, rank : 2 * rank], key_map, FIRST)
            value_sum = total[:, HEAD_DIM:] + adapter_scale * dot(
                low[j, 2 * rank : 3 * rank], value_map, FIRST
            )
            key_state[pl.ds(start, rows), :] = turned(key_sum, start, 1.0).astype(bf16)
            value_state[pl.ds(start, rows), :] = value_sum.astype(bf16)

        def block_of_head(c, j, head, block):
            lane = pl.multiple_of(head * HEAD_DIM, HEAD_DIM)
            lanes = pl.ds(lane, HEAD_DIM)
            first = pl.multiple_of(half * side_cols + c * cols + lane, HEAD_DIM)
            query_map = query_up[:, pl.ds(first, HEAD_DIM)]
            grad_map = output_down[:, pl.ds(first, HEAD_DIM)]
            start, stop = block * rows, (block + 1) * rows
            s_q, s_g = piece_of(1, c, j), piece_of(2, c, j)
            query_sum = buf[0, s_q, :, lanes].astype(f32) + own[s_q, :, lanes].astype(f32)
            query_sum += adapter_scale * dot(low[j, :rank], query_map, FIRST)
            query = turned(query_sum, start, 1.0).astype(bf16)
            grad_sum = buf[0, s_g, :, lanes].astype(f32) + own[s_g, :, lanes].astype(f32)
            out_rank = low[j, 3 * rank :]
            grad = (grad_sum + adapter_scale * dot(out_rank, grad_map, FIRST)).astype(bf16)
            key_part = key_state[:stop, :]
            value_part = value_state[:stop, :]
            scores = dot(query, key_part, LAST) * score_scale
            row = start + lax.broadcasted_iota(jnp.int32, (rows, stop), 0)
            column = lax.broadcasted_iota(jnp.int32, (rows, stop), 1)
            scores = jnp.where(row >= column, scores, -jnp.inf)
            shifted = jnp.exp(scores - jnp.max(scores, axis=1, keepdims=True))
            probs = shifted * (1.0 / jnp.sum(shifted, axis=1, keepdims=True))
            weights = probs.astype(bf16)
            attended = dot(weights, value_part).astype(bf16)
            outer[j] += dot(grad_map, attended, LAST)
            misc[c, :, lanes] += adapter_scale * dot(out_rank, attended)
            prob_grad = dot(grad, value_part, LAST)
            delta = jnp.sum(grad.astype(f32) * attended.astype(f32), axis=1, keepdims=True)
            score_grad = (probs * ((prob_grad - delta) * score_scale)).astype(bf16)
            turned_grad = turned(dot(score_grad, key_part), start, -1.0)
            back[0, back_index(c, j), :, lanes] = turned_grad.astype(bf16)
            key_grad[:stop, :] += dot(score_grad, query, FIRST)
            value_grad[:stop, :] += dot(weights, grad, FIRST)

        def attend(i):
            c = lax.div(i, 4)
            j = block_at(lax.rem(i, 4))
            piece_arrived(piece_of(1, c, j))
            piece_arrived(piece_of(2, c, j))
            here = other_index(f, j)

            def one_head(head):
                for block in range(BLOCKS):
                    pl.when(here == block)(
                        functools.partial(block_of_head, c, j, head, block)
                    )

            loop(CHUNK_HEADS, one_head)

            @pl.when((c == 0) | (j >= 2))
            def _():
                send_back(back_index(c, j))

        loop(4 * chunks, attend)
        outer_core.start()

        def send_key_value(j):
            p = back_index(chunks, j)
            start = pl.multiple_of(other_index(f, j) * rows, rows)
            key_block = turned(key_grad[pl.ds(start, rows), :], start, -1.0)
            back[0, p, :, :HEAD_DIM] = key_block.astype(bf16)
            back[0, p, :, HEAD_DIM:] = value_grad[pl.ds(start, rows), :].astype(bf16)
            send_back(p)

        send_key_value(3)
        send_key_value(2)
        for c in range(1, chunks):
            for j in range(2):
                send_back(back_index(c, j))
        send_key_value(0)
        send_key_value(1)
        outer_core.wait_recv()
        for j in range(4):
            outer_pair[j] = outer[j] + outer_got[0, j + 1 - 2 * (j % 2)]
        outer_chip.start()
        outer_chip.wait_recv()
        for j in range(4):
            passed[0, j] = (outer_pair[j] + outer_got[1, (j + 2) % 4]).astype(bf16)
        for c in range(chunks):
            passed[0, 4 + c] = misc[c].astype(bf16)
        misc_copy(0, 0, inner).start()

    def absorb(side, p):
        late = p >= far_back
        r = jnp.maximum(p - jnp.where(late, far_back, 4), 0)
        c = jnp.where(p < 4, 0, 1 + lax.div(r, 2))
        j = jnp.where(late, lax.rem(r, 2), 3 - lax.rem(r, 2))
        j = jnp.where(p < 4, block_at(p), j)
        step = min(2 * cols, width)
        for n in range(width // step):
            at = slice(n * step, (n + 1) * step)
            acc[j, :, at] += dot(back[side, p], wh[side, c, at, :], LAST)
        which = side_of(side)

        @pl.when(c < chunks)
        def _():
            column = pl.multiple_of(which * side_cols + c * cols, cols)
            rank_sum[j, :rank] += dot(query_up[:, pl.ds(column, cols)], back[side, p], LAST)
            query_acc[which * chunks + c] += dot(low[j, :rank], back[side, p])

        @pl.when(c == chunks)
        def _():
            column = pl.multiple_of(which * HEAD_DIM, HEAD_DIM)
            for i in range(2):
                values = back[side, p, :, i * HEAD_DIM : (i + 1) * HEAD_DIM]
                at = slice((i + 1) * rank, (i + 2) * rank)
                rank_sum[j, at] += dot(key_value_up[i, :, pl.ds(column, HEAD_DIM)], values, LAST)
                key_value_acc[which, i] += dot(low[j, at], values)

    def land_copy(first, count, slot, at, sem, axis, target):
        return copy(
            own.at[pl.ds(first, count)], land.at[slot, pl.ds(at, count)],
            land_send.at[sem], land_recv.at[sem], axis, target,
        )

    far_pair = land_copy(0, tiles, 1, 0, 0, "ffn", core_peer)
    near_pair = land_copy(tiles, tiles, 0, 0, 1, "ffn", core_peer)
    parts = tiles
    per_part = tiles // parts
    chip_parts = [
        land_copy(2 * tiles + n * per_part, per_part, 2, n * per_part, 2 + n, "ffn", chip_peer)
        for n in range(parts)
    ]

    def rank_core(first, sem):
        part = pl.ds(first, 2)
        return copy(
            rank_sum.at[part], rank_got.at[part], rank_send.at[sem], rank_recv.at[sem], "ffn", core_peer
        )

    def rank_chip(first, sem):
        return copy(
            rank_pair.at[pl.ds(first, 2)], rank_far.at[pl.ds(2 - first, 2)],
            rank_send.at[sem], rank_recv.at[sem], "ffn", chip_peer,
        )

    far_core, far_chip = rank_core(2, 0), rank_chip(2, 1)
    near_core, near_chip = rank_core(0, 2), rank_chip(0, 3)

    def add_pair(first):
        for j in (first, first + 1):
            rank_pair[j] = (rank_sum[j] + rank_got[j + 1 - 2 * (j % 2)]).astype(bf16)

    def back_step(t):
        def relay(h):
            v = 2 * t + h

            @pl.when((v + LAG < 2 * back_pieces) & is_mid)
            def _():
                back_arrived(0, v + LAG)
                back_across(v + LAG).start()

            @pl.when((v + LAG == 2 * back_pieces) & is_mid)
            def _():
                misc_copy(0, 0, inner).wait_recv()
                misc_copy(0, 1, inner).start()

            back_arrived(1, v)

            @pl.when(is_mid)
            def _():
                back_out(v).start()

        loop(2, relay)
        loop(2, lambda side: absorb(side, t))

        @pl.when(t == far_back - 2)
        def _():
            for n in range(tiles):
                own[n] = acc[3, :, n * cols : (n + 1) * cols].astype(bf16)
            far_pair.start()

        @pl.when(t == far_back - 1)
        def _():
            far_core.start()
            far_pair.wait_recv()
            for n in range(tiles):
                pair = acc[2, :, n * cols : (n + 1) * cols] + land[1, n].astype(f32)
                own[2 * tiles + n] = pair.astype(bf16)
            for part in chip_parts[: parts // 2]:
                part.start()

        @pl.when(t == far_back)
        def _():
            far_core.wait_recv()
            add_pair(2)
            far_chip.start()
            for part in chip_parts[parts // 2 : -1]:
                part.start()

    loop(back_pieces, back_step)
    near_core.start()
    for n in range(tiles):
        own[tiles + n] = acc[1, :, n * cols : (n + 1) * cols].astype(bf16)
    near_pair.start()

    @pl.when(is_mid)
    def _():
        misc_copy(1, 1, inner).wait_recv()
        misc_copy(1, 1, outward).start()

    near_core.wait_recv()
    add_pair(0)
    near_chip.start()
    chip_parts[-1].start()

    def put(n):
        return pltpu.make_async_copy(staged[n], results[n], result_sem.at[n])

    for c in range(2 * chunks):
        query_up_out[:, c * cols : (c + 1) * cols] = adapter_scale * query_acc[c]
    for which in range(2):
        for i in range(2):
            at = slice(which * HEAD_DIM, (which + 1) * HEAD_DIM)
            key_value_up_out[i, :, at] = adapter_scale * key_value_acc[which, i]
    put(2).start()
    put(3).start()
    far_chip.wait_recv()

    def rank_of(j):
        return (rank_pair[j].astype(f32) + rank_far[j].astype(f32)).astype(bf16)

    own_ranks = rank_of(0)
    near_pair.wait_recv()
    @pl.when(is_end)
    def _():
        misc_copy(1, 1, inner).wait_recv()

    for side in range(2):
        for c in range(chunks):
            column = pl.multiple_of(side_of(side) * side_cols + c * cols, cols)
            output_down_out[:, pl.ds(column, cols)] = passed[side, 4 + c].astype(f32)
    put(4).start()

    def outer_of(j):
        return (passed[0, j].astype(f32) + passed[1, j].astype(f32)).astype(bf16)

    total = dot(outer_of(0), up[0])
    for j in range(1, 4):
        total += dot(outer_of(j), up[j])
    output_up_out[...] = adapter_scale * total
    put(5).start()
    for which in range(2):
        for kind in range(3):
            gather(which, kind).wait_send()

    def all_sent(ref, side, sem, recv):
        copy(ref.at[side], ref.at[side], sem.at[side], recv.at[side, 0], "width", inner).wait_send()

    all_sent(buf, 1, send_sem, recv_sem)
    all_sent(back, 0, back_send, back_recv)
    low_copy(0, 0, inner).wait_send()
    misc_copy(0, 0, inner).wait_send()

    @pl.when(is_mid)
    def _():
        all_sent(buf, 0, send_sem, recv_sem)
        all_sent(back, 1, back_send, back_recv)
        low_copy(1, 0, outward).wait_send()
        misc_copy(1, 1, outward).wait_send()

    @pl.when(is_end)
    def _():
        outer_core.wait_send()
        outer_chip.wait_send()

    far_pair.wait_send()
    near_pair.wait_send()
    part_cols = per_part * cols
    put_parts = [
        pltpu.make_async_copy(
            hidden_out.at[:, pl.ds(n * part_cols, part_cols)],
            results[0].at[:, pl.ds(n * part_cols, part_cols)],
            result_sem.at[6 + n],
        )
        for n in range(parts)
    ]

    def take_part(part_index):
        chip_parts[part_index].wait_recv()
        for n in range(part_index * per_part, (part_index + 1) * per_part):
            at = slice(n * cols, (n + 1) * cols)
            terms = acc[0, :, at] + land[0, n].astype(f32) + land[2, n].astype(f32)
            adapter = adapter_scale * dot(own_ranks, down[:, at], FIRST)
            hidden_out[:, at] = (terms + adapter).astype(bf16)
        put_parts[part_index].start()

    for part_index in range(parts - 1):
        take_part(part_index)
    near_chip.wait_recv()
    total = dot(own_ranks, hid[0])
    for j in range(1, 4):
        total += dot(rank_of(j), hid[j])
    down_out[...] = adapter_scale * total
    put(1).start()
    take_part(parts - 1)
    for part in (far_core, far_chip, near_core, near_chip, *chip_parts):
        part.wait_send()
    for n in range(1, 6):
        put(n).wait()
    for part in put_parts:
        part.wait()


def pass_on(*refs):
    count = (len(refs) - 2) // 3
    sources, results, held = refs[:count], refs[count : 2 * count], refs[2 * count : 3 * count]
    in_sem, out_sem = refs[3 * count :]
    fetch = [pltpu.make_async_copy(s, h, in_sem.at[n]) for n, (s, h) in enumerate(zip(sources, held))]
    store = [pltpu.make_async_copy(h, r, out_sem.at[n]) for n, (h, r) in enumerate(zip(held, results))]
    for copy in fetch:
        copy.start()
    for arrived, copy in zip(fetch, store):
        arrived.wait()
        copy.start()
    for copy in store:
        copy.wait()


def one_kernel(
    hidden,
    upstream,
    query_frozen_weight,
    key_value_frozen_weight,
    output_frozen_weight,
    adapter_down,
    query_up_map,
    key_value_up_maps,
    output_down_map,
    output_up,
):
    bf16, f32 = jnp.bfloat16, jnp.float32
    rows, width = hidden.shape
    query_cols = query_frozen_weight.shape[1]
    cols = CHUNK_HEADS * HEAD_DIM
    chunks = query_cols // 2 // cols
    pieces = 4 + 8 * chunks
    back_pieces = 4 * chunks + 4
    tiles = width // cols
    tokens = 4 * rows
    rank = ADAPTER_RANK
    head_dims = np.arange(HEAD_DIM)
    frequency = np.exp((head_dims - head_dims % 2) * (-math.log(rope_base) / HEAD_DIM))
    angles = np.arange(tokens)[:, None] * frequency[None, :]
    cosine = jnp.asarray(np.cos(angles), f32)
    sine = jnp.asarray(np.sin(angles), f32)
    hbm = pl.BlockSpec(memory_space=pl.ANY)
    dma = pltpu.SemaphoreType.DMA
    shape = jax.ShapeDtypeStruct
    results = (
        shape((rows, width), bf16),
        shape((3 * rank, width), f32),
        shape(query_up_map.shape, f32),
        shape(key_value_up_maps.shape, f32),
        shape(output_down_map.shape, f32),
        shape(output_up.shape, f32),
    )
    held = [pltpu.VMEM(result.shape, result.dtype) for result in results]
    small = (
        cosine,
        sine,
        adapter_down.reshape(3 * rank, width),
        query_up_map,
        key_value_up_maps,
        output_down_map,
        output_up,
    )
    outputs = pl.pallas_call(
        functools.partial(fused, 1.0 / math.sqrt(HEAD_DIM)),
        out_shape=results,
        in_specs=[hbm] * 12,
        out_specs=(hbm,) * 6,
        scratch_shapes=[
            *[pltpu.VMEM(array.shape, array.dtype) for array in small],
            *held,
            pltpu.VMEM((4, rows, width), bf16),
            pltpu.VMEM((4, rows, width), bf16),
            pltpu.VMEM((2, chunks + 1, width, cols), bf16),
            pltpu.VMEM((2, 2, cols, width), bf16),
            pltpu.VMEM((2, pieces, rows, cols), bf16),
            pltpu.VMEM((pieces, rows, cols), bf16),
            pltpu.VMEM((2, back_pieces, rows, cols), bf16),
            pltpu.VMEM((4, rows, width), f32),
            pltpu.VMEM((3, tiles, rows, cols), bf16),
            pltpu.VMEM((rows, cols), f32),
            pltpu.VMEM((tokens, HEAD_DIM), bf16),
            pltpu.VMEM((tokens, HEAD_DIM), bf16),
            pltpu.VMEM((tokens, HEAD_DIM), f32),
            pltpu.VMEM((tokens, HEAD_DIM), f32),
            pltpu.VMEM((4, 4 * rank, rows), f32),
            pltpu.VMEM((2, 4, 4 * rank, rows), bf16),
            pltpu.VMEM((2, 4, 4 * rank, rows), bf16),
            pltpu.VMEM((4, 4 * rank, rows), bf16),
            pltpu.VMEM((4, 3 * rank, rows), f32),
            pltpu.VMEM((4, 3 * rank, rows), bf16),
            pltpu.VMEM((4, 3 * rank, rows), f32),
            pltpu.VMEM((4, 3 * rank, rows), bf16),
            pltpu.VMEM((4, rank, rows), f32),
            pltpu.VMEM((4, rank, rows), f32),
            pltpu.VMEM((2, 4, rank, rows), f32),
            pltpu.VMEM((chunks, rank, cols), f32),
            pltpu.VMEM((2, 4 + chunks, rank, cols), bf16),
            pltpu.VMEM((2 * chunks, rank, cols), f32),
            pltpu.VMEM((2, 2, rank, HEAD_DIM), f32),
            dma((2,)),
            dma((2, chunks + 2)),
            dma((2, 2)),
            dma((2, 3)),
            dma((2, 3)),
            dma((2,)),
            dma((2, 2 * pieces)),
            dma((2,)),
            dma((2, 2 * back_pieces)),
            dma((2,)),
            dma((2,)),
            dma((2,)),
            dma((2,)),
            dma((2,)),
            dma((2,)),
            dma((2 + tiles,)),
            dma((2 + tiles,)),
            dma((4,)),
            dma((4,)),
            dma((7,)),
            dma((6 + tiles,)),
        ],
        compiler_params=pltpu.CompilerParams(
            collective_id=0, has_side_effects=True, vmem_limit_bytes=67_000_000
        ),
    )(
        hidden,
        upstream,
        query_frozen_weight,
        key_value_frozen_weight,
        output_frozen_weight,
        *small,
    )
    outputs = pl.pallas_call(
        pass_on,
        out_shape=results,
        in_specs=[hbm] * 6,
        out_specs=(hbm,) * 6,
        scratch_shapes=[*held, dma((6,)), dma((6,))],
    )(*outputs)
    return (outputs[0], outputs[1].reshape(adapter_down.shape), *outputs[2:])


def by_shape(*arrays):
    rows, width = arrays[0].shape
    cols = CHUNK_HEADS * HEAD_DIM
    fits = (
        arrays[3].shape[2] == 2 * HEAD_DIM
        and lax.axis_size("width") == 4
        and lax.axis_size("ffn") == 4
        and arrays[2].shape[1] % (2 * cols) == 0
        and arrays[2].shape[1] >= 6 * cols
        and rows == cols
        and width % (4 * cols) == 0
    )
    return one_kernel(*arrays) if fits else shards(*arrays)


def solution(mesh):
    placed = (
        P(("groups", "ffn"), "width"),
        P(("groups", "ffn"), "width"),
        P("width", "ffn"),
        P(None, "width", "ffn"),
        P("ffn", "width"),
        P("groups", None, "width"),
        P("groups", "ffn"),
        P("groups", None, "ffn"),
        P("groups", "ffn"),
        P("groups", "width"),
    )
    return jax.shard_map(
        by_shape,
        mesh=mesh,
        in_specs=placed,
        out_specs=(
            P(("groups", "ffn"), "width"),
            P("groups", None, "width"),
            P("groups", "ffn"),
            P("groups", None, "ffn"),
            P("groups", "ffn"),
            P("groups", "width"),
        ),
        check_vma=False,
    )
```
